32 devices in a mesh: tp: 4 (over z), dp: 8 (over y, x, core).
Axes of the slice: x: 2, y: 2, z: 4, core: 2. Of those that a mesh axis runs over, the one named last changes fastest.
Arguments:
- g_qkv: bfloat16 [8, 1024, 32, 3, 80], P('dp', None, 'tp')
- g_out: bfloat16 [8, 2560, 1024], P('dp', 'tp')
- g_up: bfloat16 [8, 1024, 4096], P('dp', None, 'tp')
- g_down: bfloat16 [8, 4096, 1024], P('dp', 'tp')
- g_norms: bfloat16 [8, 6, 1024], P('dp')
- master: float32 [4, 4724736], P('tp', 'dp')
- mom_one: float32 [4, 4724736], P('tp', 'dp')
- mom_two: float32 [4, 4724736], P('tp', 'dp')
Outputs:
- output 1: bfloat16 [1024, 32, 3, 80], P(None, 'tp')
- output 2: bfloat16 [2560, 1024], P('tp')
- output 3: bfloat16 [1024, 4096], P(None, 'tp')
- output 4: bfloat16 [4096, 1024], P('tp')
- output 5: bfloat16 [6, 1024], replicated
- output 6: float32 [4, 4724736], P('tp', 'dp')
- output 7: float32 [4, 4724736], P('tp', 'dp')
- output 8: float32 [4, 4724736], P('tp', 'dp')
- output 9: float32 [], replicated
All inputs are finite; a program needn't handle non-finite values.
Results may differ from the reference program's by a relative error of at most 0.001.
Values are sent between devices in bfloat16 or wider.
A program may use at most 1 GiB of HBM per device.

```python
import jax
import jax.numpy as jnp
from jax import lax

WIDTH = 1024
HEADS = 32
KV_HEADS = 32
HEAD = 80
FF_RED = 4096
TP_SIZE = 4
DP_SIZE = 8
STEP = 20

QKV_SLOTS = HEADS // KV_HEADS + 2
KV_LOCAL = KV_HEADS // TP_SIZE
FF_LOCAL = FF_RED // TP_SIZE
QKV_END = WIDTH * KV_LOCAL * QKV_SLOTS * HEAD
OUT_END = QKV_END + (HEADS * HEAD // TP_SIZE) * WIDTH
UP_END = OUT_END + WIDTH * FF_LOCAL
MAT_COUNT = UP_END + FF_LOCAL * WIDTH
LN_COUNT = 6 * WIDTH
FLAT_COUNT = MAT_COUNT + LN_COUNT
BETA_ONE = 0.9
BETA_TWO = 0.95
ADAM_EPS = 1e-8
DECAY = 0.1
LEARN_RATE = 1e-4
MAX_NORM = 1.0
NORM_EPS = 1e-6
BIAS_ONE = 1.0 - BETA_ONE ** STEP
BIAS_TWO = 1.0 - BETA_TWO ** STEP
GRAD_MAT_STD = (8.0 * DP_SIZE / (TP_SIZE * MAT_COUNT)) ** 0.5
GRAD_LN_STD = (8.0 * DP_SIZE / LN_COUNT) ** 0.5
CLIP_MAT_STD = (0.5 / (TP_SIZE * MAT_COUNT)) ** 0.5
CLIP_LN_STD = (0.5 / LN_COUNT) ** 0.5


def to_flat(w_qkv, w_out, w_up, w_down, w_norms):
    qkv_rows = w_qkv.reshape(WIDTH, TP_SIZE, KV_LOCAL, QKV_SLOTS, HEAD).transpose(1, 0, 2, 3, 4).reshape(TP_SIZE, QKV_END)
    out_rows = w_out.reshape(TP_SIZE, OUT_END - QKV_END)
    up_rows = w_up.reshape(WIDTH, TP_SIZE, FF_LOCAL).transpose(1, 0, 2).reshape(TP_SIZE, UP_END - OUT_END)
    down_rows = w_down.reshape(TP_SIZE, MAT_COUNT - UP_END)
    norm_rows = jnp.broadcast_to(w_norms.reshape(1, LN_COUNT), (TP_SIZE, LN_COUNT))
    return jnp.concatenate([qkv_rows, out_rows, up_rows, down_rows, norm_rows], axis=1)


def from_flat(flat):
    p_qkv = flat[:, :QKV_END].reshape(TP_SIZE, WIDTH, KV_LOCAL, QKV_SLOTS, HEAD).transpose(1, 0, 2, 3, 4).reshape(WIDTH, KV_HEADS, QKV_SLOTS, HEAD)
    p_out = flat[:, QKV_END:OUT_END].reshape(HEADS * HEAD, WIDTH)
    p_up = flat[:, OUT_END:UP_END].reshape(TP_SIZE, WIDTH, FF_LOCAL).transpose(1, 0, 2).reshape(WIDTH, FF_RED)
    p_down = flat[:, UP_END:MAT_COUNT].reshape(FF_RED, WIDTH)
    p_norms = flat[0, MAT_COUNT:].reshape(6, WIDTH)
    return p_qkv, p_out, p_up, p_down, p_norms


def replica_mean(grad):
    total = lax.fori_loop(0, DP_SIZE, lambda index, running: running + grad[index].astype(jnp.float32), jnp.zeros(grad.shape[1:], jnp.float32))
    return total / DP_SIZE


def draw_replicas(key, shape, scale):
    def one_replica(sub_key):
        return (jax.random.normal(sub_key, shape, jnp.float32) * scale).astype(jnp.bfloat16)
    return lax.map(one_replica, jax.random.split(key, DP_SIZE))


def setup_inputs(seed: int = 0) -> dict:
    keys = jax.random.split(jax.random.key(seed), 16)
    qkv_shape = (WIDTH, KV_HEADS, QKV_SLOTS, HEAD)
    out_shape = (HEADS * HEAD, WIDTH)
    up_shape = (WIDTH, FF_RED)
    down_shape = (FF_RED, WIDTH)
    g_qkv = draw_replicas(keys[0], qkv_shape, GRAD_MAT_STD)
    g_out = draw_replicas(keys[1], out_shape, GRAD_MAT_STD)
    g_up = draw_replicas(keys[2], up_shape, GRAD_MAT_STD)
    g_down = draw_replicas(keys[3], down_shape, GRAD_MAT_STD)
    g_norms = draw_replicas(keys[4], (6, WIDTH), GRAD_LN_STD)
    w_qkv = jax.random.normal(keys[5], qkv_shape, jnp.float32) * WIDTH ** -0.5
    w_out = jax.random.normal(keys[6], out_shape, jnp.float32) * (HEADS * HEAD) ** -0.5
    w_up = jax.random.normal(keys[7], up_shape, jnp.float32) * WIDTH ** -0.5
    w_down = jax.random.normal(keys[8], down_shape, jnp.float32) * FF_RED ** -0.5
    norm_base = jnp.tile(jnp.array([1.0, 0.0], jnp.float32), 3).reshape(6, 1)
    w_norms = norm_base + 0.1 * jax.random.normal(keys[9], (6, WIDTH), jnp.float32)
    master = to_flat(w_qkv, w_out, w_up, w_down, w_norms)
    mom_mat = 0.2 * CLIP_MAT_STD * jax.random.normal(keys[10], (TP_SIZE, MAT_COUNT), jnp.float32)
    mom_ln = 0.2 * CLIP_LN_STD * jax.random.normal(keys[11], (1, LN_COUNT), jnp.float32)
    mom_one = jnp.concatenate([mom_mat, jnp.broadcast_to(mom_ln, (TP_SIZE, LN_COUNT))], axis=1)
    var_mat = CLIP_MAT_STD * CLIP_MAT_STD * jax.random.uniform(keys[12], (TP_SIZE, MAT_COUNT), jnp.float32, 0.5, 1.5)
    var_ln = CLIP_LN_STD * CLIP_LN_STD * jax.random.uniform(keys[13], (1, LN_COUNT), jnp.float32, 0.5, 1.5)
    mom_two = jnp.concatenate([var_mat, jnp.broadcast_to(var_ln, (TP_SIZE, LN_COUNT))], axis=1)
    return {"g_qkv": g_qkv, "g_out": g_out, "g_up": g_up, "g_down": g_down, "g_norms": g_norms, "master": master, "mom_one": mom_one, "mom_two": mom_two}


def reference(g_qkv, g_out, g_up, g_down, g_norms, master, mom_one, mom_two):
    means = [replica_mean(grad) for grad in (g_qkv, g_out, g_up, g_down, g_norms)]
    grad_norm = jnp.sqrt(sum(jnp.sum(mean_grad * mean_grad) for mean_grad in means))
    clip = jnp.minimum(1.0, MAX_NORM / (grad_norm + NORM_EPS))
    grad_flat = to_flat(means[0], means[1], means[2], means[3], means[4]) * clip
    is_matrix = (jnp.arange(FLAT_COUNT) < MAT_COUNT)[None, :]
    mom_one_new = BETA_ONE * mom_one + (1.0 - BETA_ONE) * grad_flat
    mom_two_new = BETA_TWO * mom_two + (1.0 - BETA_TWO) * grad_flat * grad_flat
    step_dir = (mom_one_new / BIAS_ONE) / (jnp.sqrt(mom_two_new / BIAS_TWO) + ADAM_EPS)
    master_new = master - LEARN_RATE * (step_dir + jnp.where(is_matrix, DECAY * master, 0.0))
    p_qkv, p_out, p_up, p_down, p_norms = from_flat(master_new.astype(jnp.bfloat16))
    return (p_qkv, p_out, p_up, p_down, p_norms, master_new, mom_one_new, mom_two_new, grad_norm)
```

```python
import functools

import jax
import jax.numpy as jnp
from jax import lax
from jax.experimental import pallas as pl
from jax.experimental.pallas import tpu as pltpu
from jax.sharding import PartitionSpec as P

STEP = 20
BETA_ONE = 0.9
BETA_TWO = 0.95
ADAM_EPS = 1e-8
DECAY = 0.1
LEARN_RATE = 1e-4
MAX_NORM = 1.0
NORM_EPS = 1e-6
BIAS_ONE = 1.0 - BETA_ONE ** STEP
BIAS_TWO = 1.0 - BETA_TWO ** STEP
ARG_SPECS = (P("dp", None, "tp", None, None), P("dp", "tp", None), P("dp", None, "tp"), P("dp", "tp", None), P("dp", None, None), P("tp", "dp"), P("tp", "dp"), P("tp", "dp"))
OUT_SPECS = (P(None, "tp", None, None), P("tp", None), P(None, "tp"), P("tp", None), P(None, None), P("tp", "dp"), P("tp", "dp"), P("tp", "dp"), P())

MESH = pl.DeviceIdType.MESH
F32 = jnp.float32
BF16 = jnp.bfloat16

Q_TILES = 1920
TILES = 4616
Q_COLS = 15
M_COLS = 8
PART_ROWS = 4614
MAT_ROWS = 36864
WIN = 600
HALF = WIN // 2
WIN_START = (0, 570, 1140, 1725, 2304, 2880, 3456, 4016)
EMIT_START = (0, 585, 1155, 1740, 2312, 2888, 3464, 4040)
EMIT_END = (585, 1155, 1740, 2312, 2888, 3464, 4040, 4616)
Q_BLOCKS = (40, 40, 40, 13, 0, 0, 0, 0)
M_BLOCKS = (0, 0, 0, 50, 75, 75, 75, 75)
EMIT = 588
STATE_BASE = 176
STATE_ROWS = 4984
HALO = 80

K_RS = 5
N_RS = HALF // K_RS
K_AG = 6
N_AG = EMIT // K_AG
STEP_TILES = 4


def pick(values, y, x, c):
    total = 0
    for index, value in enumerate(values):
        if value:
            term = value
            for shift, bit in ((2, y), (1, x), (0, c)):
                term = term * (bit if (index >> shift) & 1 else 1 - bit)
            total = total + term
    return total


def step_kernel(gq, go, gu, gd, gn, w_in, m_in, v_in,
                ag, w_out, m_out, v_out, norm_out,
                grads, r_ra, r_rb, r_da, r_db, r_pf, r_pa, r_pb,
                r_sa, r_sb, s_sa, s_sb, gsum, mask, state, halo, pbuf, nb1, nb2,
                load_sem, store_sem, own_sem,
                ss_raw, rs_raw, ss_pf, rs_pf, ss_pp, rs_pp, ss_s, rs_s,
                ss_h, rs_h, ss_n1, rs_n1, ss_n2, rs_n2,
                ss_own, rs_own, ss_rel, rs_rel, ss_d2d, rs_d2d):
    dp = lax.axis_index("dp")
    tp = lax.axis_index("tp")
    y = dp // 4
    x = dp // 2 % 2
    c = dp % 2

    def at(yy, xx, cc):
        return {"dp": yy * 4 + xx * 2 + cc}

    def win(yy, xx, cc):
        return pick(WIN_START, yy, xx, cc)

    ny, nx, nc = 1 - y, 1 - x, 1 - c

    def remote(src, dst, ssem, rsem, dev):
        return pltpu.make_async_remote_copy(
            src_ref=src, dst_ref=dst, send_sem=ssem, recv_sem=rsem, device_id=dev, device_id_type=MESH)

    loads = []
    for index, (src, start, count) in enumerate((
            (gq, 0, 1920), (go, 1920, 640), (gu, 2560, 1024), (gd, 3584, 1024), (gn, 4608, 8))):
        loads.append(pltpu.make_async_copy(src, grads.at[pl.ds(start, count)], load_sem.at[index]))
    state_loads = []
    for index, src in enumerate((w_in, m_in, v_in)):
        state_loads.append(pltpu.make_async_copy(
            src, state.at[index, pl.ds(STATE_BASE, PART_ROWS)], load_sem.at[5 + index]))
    for copy in loads:
        copy.start()
    barrier = pltpu.get_barrier_semaphore()
    for offset in range(1, 8):
        pl.semaphore_signal(barrier, inc=1, device_id={"dp": (dp + offset) % 8}, device_id_type=MESH)
    for offset in range(1, 4):
        pl.semaphore_signal(barrier, inc=1, device_id={"tp": (tp + offset) % 4}, device_id_type=MESH)
    pl.semaphore_wait(barrier, 10)
    for copy in loads:
        copy.wait()

    def cut(start, k, n=N_RS):
        return pl.ds(start + k * n, n)

    raw_bufs = (r_ra, r_rb, r_da, r_db)

    def raw(stream, cc, k, slot):
        to_y = stream in (0, 2)
        half = 0 if to_y else HALF
        if stream < 2:
            start = win(ny, nx, cc)
        elif to_y:
            start = win(ny, x, cc)
        else:
            start = win(y, nx, cc)
        dev = at(ny, x, cc) if to_y else at(y, nx, cc)
        return remote(grads.at[cut(start + half, k)], raw_bufs[stream].at[slot, cut(0, k)],
                      ss_raw.at[stream, cc, k], rs_raw.at[stream, slot, k], dev)

    def partner_final(k):
        return remote(grads.at[cut(win(y, x, nc), k)], r_pf.at[cut(0, k)], ss_pf.at[k], rs_pf.at[k], at(y, x, nc))

    def partner_relay(which, k):
        if which == 0:
            start, dst = win(y, nx, nc), r_pa
        else:
            start, dst = win(ny, x, nc) + HALF, r_pb
        return remote(grads.at[cut(start, k)], dst.at[cut(0, k)], ss_pp.at[which, k], rs_pp.at[which, k], at(y, x, nc))

    def relayed(which, k):
        src, dst, dev = (s_sa, r_sa, at(y, nx, c)) if which == 0 else (s_sb, r_sb, at(ny, x, c))
        return remote(src.at[cut(0, k)], dst.at[cut(0, k)], ss_s.at[which, k], rs_s.at[which, k], dev)

    def halo_copy(index):
        src = (w_in, m_in, v_in)[index]
        return remote(src.at[pl.ds(0, HALO)], halo.at[index],
                      ss_h.at[index], rs_h.at[index], {"dp": (dp + 7) % 8})

    def send_relay_raw(k, carry):
        for cc in range(2):
            raw(0, cc, k, c).start()
            raw(1, cc, k, c).start()
        partner_relay(0, k).start()
        partner_relay(1, k).start()
        return carry

    def send_direct_raw(k, carry):
        for cc in range(2):
            raw(2, cc, k, c).start()
            raw(3, cc, k, c).start()
        partner_final(k).start()
        partner_final(k + K_RS).start()
        return carry

    lax.fori_loop(0, K_RS, send_relay_raw, 0)
    lax.fori_loop(0, K_RS, send_direct_raw, 0)
    for index in range(3):
        halo_copy(index).start()
    for copy in state_loads:
        copy.start()

    off = PART_ROWS * dp - 8 * win(y, x, c)
    mat_end = MAT_ROWS - 8 * win(y, x, c)
    last = jnp.minimum(off + PART_ROWS, mat_end + jnp.where(tp == 0, 48, 0))
    q_blocks = pick(Q_BLOCKS, y, x, c)
    m_blocks = pick(M_BLOCKS, y, x, c)
    row = lax.broadcasted_iota(jnp.int32, (8, 128), 0)
    for index in range(WIN - 5, WIN):
        mask[index] = jnp.zeros((8, 128), F32)

    def mask_blocks(columns, tile0):
        def body(block, carry):
            for col in range(columns):
                tile = tile0 + block * columns + col
                lane_row = row * columns + (tile0 * 8 + block * columns * 8 + col)
                inside = jnp.logical_and(lane_row >= off, lane_row < last)
                mask[tile] = jnp.where(inside, 1.0, 0.0)
            return carry
        return body

    lax.fori_loop(0, q_blocks, mask_blocks(Q_COLS, 0), 0)
    lax.fori_loop(0, m_blocks, mask_blocks(M_COLS, q_blocks * Q_COLS), 0)

    def relay(which):
        own_start = win(y, nx, c) if which == 0 else win(ny, x, c) + HALF
        raw_buf, pair_buf, out_buf = (r_ra, r_pa, s_sa) if which == 0 else (r_rb, r_pb, s_sb)

        def body(k):
            raw(which, 0, k, 0).wait_recv()
            raw(which, 1, k, 1).wait_recv()
            partner_relay(which, k).wait_recv()

            def tiles(index, carry):
                here = pl.ds(k * N_RS + index * STEP_TILES, STEP_TILES)
                total = grads[pl.ds(own_start + k * N_RS + index * STEP_TILES, STEP_TILES)].astype(F32)
                total = total + pair_buf[here].astype(F32)
                total = total + raw_buf[0, here].astype(F32)
                total = total + raw_buf[1, here].astype(F32)
                out_buf[here] = total
                return carry

            lax.fori_loop(0, N_RS // STEP_TILES, tiles, 0)
            relayed(which, k).start()
        return body

    relay_a, relay_b = relay(0), relay(1)

    def relay_step(k, carry):
        relay_a(k)
        relay_b(k)
        return carry

    lax.fori_loop(0, K_RS, relay_step, 0)

    for copy in state_loads:
        copy.wait()
    for index in range(3):
        halo_copy(index).wait_recv()
        state[index, pl.ds(STATE_BASE + PART_ROWS, HALO)] = halo[index]

    def finish(which):
        half = 0 if which == 0 else HALF
        raw_buf, sum_buf = (r_da, r_sa) if which == 0 else (r_db, r_sb)

        def body(k, acc):
            raw(2 + which, 0, k, 0).wait_recv()
            raw(2 + which, 1, k, 1).wait_recv()
            partner_final(k + which * K_RS).wait_recv()
            relayed(which, k).wait_recv()

            def tiles(index, acc):
                here = pl.ds(k * N_RS + index * STEP_TILES, STEP_TILES)
                part = pl.ds(half + k * N_RS + index * STEP_TILES, STEP_TILES)
                total = grads[pl.ds(win(y, x, c) + half + k * N_RS + index * STEP_TILES, STEP_TILES)].astype(F32)
                total = total + r_pf[part].astype(F32)
                total = total + raw_buf[0, here].astype(F32)
                total = total + raw_buf[1, here].astype(F32)
                total = (total + sum_buf[here]) * 0.125
                gsum[part] = total
                square = jnp.where(mask[part] > 0.5, total * total, 0.0)
                return acc + jnp.sum(square, axis=0)

            return lax.fori_loop(0, N_RS // STEP_TILES, tiles, acc)
        return body

    finish_a, finish_b = finish(0), finish(1)
    acc = lax.fori_loop(0, K_RS, lambda k, acc: finish_b(k, finish_a(k, acc)), jnp.zeros((8, 128), F32))

    nb1[dp] = acc

    def norm_plane(offset):
        return remote(nb1.at[dp], nb1.at[dp], ss_n1.at[offset], rs_n1.at[dp], {"dp": (dp + offset) % 8})

    def norm_plane_in(offset):
        source = (dp + offset) % 8
        return remote(nb1.at[dp], nb1.at[source], ss_n1.at[offset], rs_n1.at[source], {"dp": source})

    def norm_line(offset):
        return remote(nb2.at[tp], nb2.at[tp], ss_n2.at[offset], rs_n2.at[tp], {"tp": (tp + offset) % 4})

    def norm_line_in(offset):
        source = (tp + offset) % 4
        return remote(nb2.at[tp], nb2.at[source], ss_n2.at[offset], rs_n2.at[source], {"tp": source})

    for offset in range(1, 8):
        norm_plane(offset).start()
    for offset in range(1, 8):
        norm_plane_in(offset).wait_recv()
    plane = nb1[0]
    for index in range(1, 8):
        plane = plane + nb1[index]
    nb2[tp] = plane
    for offset in range(1, 4):
        norm_line(offset).start()
    for offset in range(1, 4):
        norm_line_in(offset).wait_recv()
    total = nb2[0] + nb2[1] + nb2[2] + nb2[3]
    total = jnp.sum(jnp.sum(total, axis=0, keepdims=True), axis=1, keepdims=True)
    norm = jnp.sqrt(jnp.broadcast_to(total, (8, 128)))
    norm_out[...] = norm
    clip = jnp.minimum(1.0, MAX_NORM / (norm + NORM_EPS))

    def update_blocks(columns, tile0):
        def body(block, carry):
            row0 = tile0 * 8 + block * columns * 8
            decay = jnp.where(row0 < mat_end, DECAY, 0.0)
            for col in range(columns):
                tile = tile0 + block * columns + col
                here = pl.ds(STATE_BASE - off + row0 + col, 8, stride=columns)
                grad = gsum[tile] * clip
                w_old = state[0, here]
                m_new = BETA_ONE * state[1, here] + (1.0 - BETA_ONE) * grad
                v_new = BETA_TWO * state[2, here] + (1.0 - BETA_TWO) * grad * grad
                step_dir = (m_new * (1.0 / BIAS_ONE)) / (jnp.sqrt(v_new * (1.0 / BIAS_TWO)) + ADAM_EPS)
                w_new = w_old - LEARN_RATE * (step_dir + decay * w_old)
                state[0, here] = w_new
                state[1, here] = m_new
                state[2, here] = v_new
                pbuf[tile] = w_new.astype(BF16)
            return carry
        return body

    lax.fori_loop(0, q_blocks, update_blocks(Q_COLS, 0), 0)
    lax.fori_loop(0, m_blocks, update_blocks(M_COLS, q_blocks * Q_COLS), 0)

    emit0 = pick([e - s for e, s in zip(EMIT_START, WIN_START)], y, x, c)

    def piece(k):
        return pl.ds(k * N_AG, N_AG)

    def own_out(which, k):
        dev = (at(y, nx, c), at(ny, x, c), at(y, x, nc))[which]
        return remote(pbuf.at[pl.ds(emit0 + k * N_AG, N_AG)], ag.at[dp, piece(k)],
                      ss_own.at[which, k], rs_own.at[which, k], dev)

    def own_in(which, k):
        part = (y * 4 + nx * 2 + c, ny * 4 + x * 2 + c, y * 4 + x * 2 + nc)[which]
        dev = (at(y, nx, c), at(ny, x, c), at(y, x, nc))[which]
        return remote(ag.at[part, piece(k)], ag.at[part, piece(k)], ss_own.at[which, k], rs_own.at[which, k], dev)

    def pass_out(which, k):
        if which == 0:
            part, dev = y * 4 + nx * 2 + c, at(ny, x, c)
        else:
            part, dev = ny * 4 + x * 2 + c, at(y, nx, c)
        return remote(ag.at[part, piece(k)], ag.at[part, piece(k)], ss_rel.at[k], rs_rel.at[k], dev)

    def pass_in(which, k):
        part = ny * 4 + nx * 2 + c
        dev = at(ny, x, c) if which == 0 else at(y, nx, c)
        return remote(ag.at[part, piece(k)], ag.at[part, piece(k)], ss_rel.at[k], rs_rel.at[k], dev)

    def pair_out(which, k):
        part = (y * 4 + nx * 2 + c, ny * 4 + x * 2 + c, ny * 4 + nx * 2 + c)[which]
        return remote(ag.at[part, piece(k)], ag.at[part, piece(k)], ss_d2d.at[which, k], rs_d2d.at[which, k], at(y, x, nc))

    def pair_in(which, k):
        part = (y * 4 + nx * 2 + nc, ny * 4 + x * 2 + nc, ny * 4 + nx * 2 + nc)[which]
        return remote(ag.at[part, piece(k)], ag.at[part, piece(k)], ss_d2d.at[which, k], rs_d2d.at[which, k], at(y, x, nc))

    own_copy = pltpu.make_async_copy(pbuf.at[pl.ds(emit0, EMIT)], ag.at[dp], own_sem)
    half_ag = K_AG // 2

    def send_own(index, carry):
        own_out(0, index).start()
        own_out(1, (index + half_ag) % K_AG).start()
        return carry

    lax.fori_loop(0, K_AG, send_own, 0)
    own_copy.start()
    lax.fori_loop(0, K_AG, lambda k, carry: (own_out(2, k).start(), carry)[1], 0)
    stores = []
    for index, dst in enumerate((w_out, m_out, v_out)):
        stores.append(pltpu.make_async_copy(
            state.at[index, pl.ds(STATE_BASE, PART_ROWS)], dst, store_sem.at[index]))
        stores[-1].start()

    def first_half(k, carry):
        own_in(0, k).wait_recv()
        pass_out(0, k).start()
        pair_out(0, k).start()
        own_in(1, k + half_ag).wait_recv()
        pass_out(1, k + half_ag).start()
        pair_out(1, k + half_ag).start()
        return carry

    def second_half(k, carry):
        own_in(0, k + half_ag).wait_recv()
        pair_out(0, k + half_ag).start()
        own_in(1, k).wait_recv()
        pair_out(1, k).start()
        return carry

    def diagonal(k, carry):
        pass_in(0, k).wait_recv()
        pair_out(2, k).start()
        pass_in(1, k + half_ag).wait_recv()
        pair_out(2, k + half_ag).start()
        return carry

    lax.fori_loop(0, half_ag, first_half, 0)
    lax.fori_loop(0, half_ag, second_half, 0)
    lax.fori_loop(0, half_ag, diagonal, 0)

    def drain_ag(k, carry):
        own_in(2, k).wait_recv()
        for which in range(3):
            pair_in(which, k).wait_recv()
            pair_out(which, k).wait_send()
            own_out(which, k).wait_send()
        return carry

    lax.fori_loop(0, K_AG, drain_ag, 0)

    def drain_half(k, carry):
        pass_out(0, k).wait_send()
        pass_out(1, k + half_ag).wait_send()
        return carry

    lax.fori_loop(0, half_ag, drain_half, 0)

    def drain_rs(k, carry):
        for stream in range(4):
            for cc in range(2):
                raw(stream, cc, k, c).wait_send()
        partner_final(k).wait_send()
        partner_final(k + K_RS).wait_send()
        for which in range(2):
            partner_relay(which, k).wait_send()
            relayed(which, k).wait_send()
        return carry

    lax.fori_loop(0, K_RS, drain_rs, 0)
    for index in range(3):
        halo_copy(index).wait_send()
    for offset in range(1, 8):
        norm_plane(offset).wait_send()
    for offset in range(1, 4):
        norm_line(offset).wait_send()
    own_copy.wait()
    for copy in stores:
        copy.wait()


def lay_out_kernel(ag, q_out, o_out, u_out, d_out, n_out, tiles, in_sem, out_sem):
    loads = []
    for part in range(8):
        start, end = EMIT_START[part], EMIT_END[part]
        loads.append(pltpu.make_async_copy(
            ag.at[part, pl.ds(0, end - start)], tiles.at[pl.ds(start, end - start)], in_sem.at[part]))
        loads[-1].start()
    outs = []
    for index, (dst, start, count) in enumerate((
            (q_out, 0, 1920), (o_out, 1920, 640), (u_out, 2560, 1024), (d_out, 3584, 1024), (n_out, 4608, 8))):
        outs.append(pltpu.make_async_copy(tiles.at[pl.ds(start, count)], dst, out_sem.at[index]))
    for part in range(8):
        loads[part].wait()
        if part == 3:
            outs[0].start()
        if part == 5:
            outs[1].start()
        if part == 6:
            outs[2].start()
    outs[3].start()
    outs[4].start()
    for copy in outs:
        copy.wait()


def to_tiles(matrix):
    rows, cols = matrix.shape
    return matrix.reshape(rows // 8, 8, cols // 128, 128).transpose(0, 2, 1, 3).reshape(rows * cols // 1024, 8, 128)


def from_tiles(tiles, rows, cols):
    return tiles.reshape(rows // 8, cols // 128, 8, 128).transpose(0, 2, 1, 3).reshape(rows, cols)


def any_spec(count):
    return [pl.BlockSpec(memory_space=pl.ANY)] * count


def solution(mesh):
    dma = pltpu.SemaphoreType.DMA

    def local_step(g_qkv, g_out, g_up, g_down, g_norms, master, mom_one, mom_two):
        gq = to_tiles(g_qkv[0].transpose(1, 2, 3, 0).reshape(1920, 1024).T)
        go, gu, gd = to_tiles(g_out[0]), to_tiles(g_up[0]), to_tiles(g_down[0])
        gn = to_tiles(jnp.pad(g_norms[0], ((0, 2), (0, 0))))
        part = jax.ShapeDtypeStruct((PART_ROWS, 128), F32)
        scratch = [
            pltpu.VMEM((TILES, 8, 128), BF16),
            *[pltpu.VMEM((2, HALF, 8, 128), BF16)] * 4,
            pltpu.VMEM((WIN, 8, 128), BF16),
            *[pltpu.VMEM((HALF, 8, 128), BF16)] * 2,
            *[pltpu.VMEM((HALF, 8, 128), F32)] * 4,
            pltpu.VMEM((WIN, 8, 128), F32),
            pltpu.VMEM((WIN, 8, 128), F32),
            pltpu.VMEM((3, STATE_ROWS, 128), F32),
            pltpu.VMEM((3, HALO, 128), F32),
            pltpu.VMEM((616, 8, 128), BF16),
            pltpu.VMEM((8, 8, 128), F32),
            pltpu.VMEM((4, 8, 128), F32),
            dma((8,)), dma((3,)), dma(()),
            dma((4, 2, K_RS)), dma((4, 2, K_RS)),
            dma((2 * K_RS,)), dma((2 * K_RS,)),
            dma((2, K_RS)), dma((2, K_RS)),
            dma((2, K_RS)), dma((2, K_RS)),
            dma((3,)), dma((3,)),
            dma((8,)), dma((8,)),
            dma((4,)), dma((4,)),
            dma((3, K_AG)), dma((3, K_AG)),
            dma((K_AG,)), dma((K_AG,)),
            dma((3, K_AG)), dma((3, K_AG)),
        ]
        ag, w_new, m_new, v_new, norm = pl.pallas_call(
            step_kernel,
            name="reduce_update_gather",
            out_shape=[jax.ShapeDtypeStruct((8, EMIT, 8, 128), BF16), part, part, part,
                       jax.ShapeDtypeStruct((8, 128), F32)],
            in_specs=any_spec(8),
            out_specs=any_spec(4) + [pl.BlockSpec(memory_space=pltpu.VMEM)],
            scratch_shapes=scratch,
            compiler_params=pltpu.CompilerParams(
                collective_id=0, has_side_effects=True, vmem_limit_bytes=60 * 1024 * 1024),
        )(gq, go, gu, gd, gn, *[a.reshape(PART_ROWS, 128) for a in (master, mom_one, mom_two)])
        w_new, m_new, v_new = [a.reshape(master.shape) for a in (w_new, m_new, v_new)]
        pq, po, pu, pd, pn = pl.pallas_call(
            lay_out_kernel,
            name="lay_out",
            out_shape=[jax.ShapeDtypeStruct((count, 8, 128), BF16) for count in (1920, 640, 1024, 1024, 8)],
            in_specs=any_spec(1),
            out_specs=any_spec(5),
            scratch_shapes=[pltpu.VMEM((TILES, 8, 128), BF16), dma((8,)), dma((5,))],
            compiler_params=pltpu.CompilerParams(vmem_limit_bytes=32 * 1024 * 1024),
        )(ag)
        p_qkv = from_tiles(pq, 1024, 1920).T.reshape(8, 3, 80, 1024).transpose(3, 0, 1, 2)
        return (p_qkv, from_tiles(po, 640, 1024), from_tiles(pu, 1024, 1024), from_tiles(pd, 1024, 1024),
                from_tiles(pn, 8, 1024)[:6], w_new, m_new, v_new, norm[0, 0])

    return jax.shard_map(local_step, mesh=mesh, in_specs=ARG_SPECS, out_specs=OUT_SPECS, check_vma=False)
```

```python
import functools

import jax
import jax.numpy as jnp
from jax import lax
from jax.experimental import pallas as pl
from jax.experimental.pallas import tpu as pltpu
from jax.sharding import PartitionSpec as P

STEP = 20
BETA_ONE = 0.9
BETA_TWO = 0.95
ADAM_EPS = 1e-8
DECAY = 0.1
LEARN_RATE = 1e-4
MAX_NORM = 1.0
NORM_EPS = 1e-6
BIAS_ONE = 1.0 - BETA_ONE ** STEP
BIAS_TWO = 1.0 - BETA_TWO ** STEP
TP_COL = P(None, "tp")
ROW_DP = P("dp")
STATE = P("tp", "dp")
ARG_SPECS = (P("dp", None, "tp"), P("dp", "tp"), P("dp", None, "tp"), P("dp", "tp"), ROW_DP, STATE, STATE, STATE)
OUT_SPECS = (TP_COL, P("tp"), TP_COL, P("tp"), P(), STATE, STATE, STATE, P())

MESH = pl.DeviceIdType.MESH
F32 = jnp.float32
BF16 = jnp.bfloat16

Q_TILES = 1920
TILES = 4616
Q_COLS = 15
M_COLS = 8
PART_ROWS = 4614
MAT_ROWS = 36864
WIN = 600
HALF = WIN // 2
WIN_START = (0, 570, 1140, 1725, 2304, 2880, 3456, 4016)
EMIT_START = (0, 585, 1155, 1740, 2312, 2888, 3464, 4040)
EMIT_END = (585, 1155, 1740, 2312, 2888, 3464, 4040, 4616)
Q_BLOCKS = (40, 40, 40, 13, 0, 0, 0, 0)
M_BLOCKS = (0, 0, 0, 50, 75, 75, 75, 75)
EMIT = 588
STATE_BASE = 176
STATE_ROWS = 4984
HALO = 80

K_RS = 5
N_RS = HALF // K_RS
K_AG = 12
N_AG = EMIT // K_AG
STEP_TILES = 4
HALF_AG = K_AG // 2
FLAT = PART_ROWS * 128
CHUNK_ROWS = 64
CHUNK = CHUNK_ROWS * 128
CHUNKS = PART_ROWS // CHUNK_ROWS
TAIL = PART_ROWS - CHUNKS * CHUNK_ROWS
TILE = (8, 128)
VMEM_LIMIT = 50 * 1024 * 1024
STEP_VMEM = 50 * 1024 * 1024
DP, TP = 8, 4
O_START, U_START, D_START, N_START = 1920, 2560, 3584, 4608
S_RAW, S_PF, S_PP, S_SUM, S_HALO, S_N1, S_N2, S_OWN, S_PAIR, S_PASS, SENDS = 0, 8, 9, 11, 13, 16, 17, 18, 21, 24, 25


def fori(count, step, start=0):
    def body(k, carry):
        step(k)
        return carry

    lax.fori_loop(start, count, body, 0)


def lanes(block):
    return pl.ds(pl.multiple_of(block * 128, 128), 128)


PIECE_ORDER = tuple(k // 2 + (K_AG // 2) * (k % 2) for k in range(K_AG))


def piece_blocks():
    table = []
    for k, piece in enumerate(PIECE_ORDER):
        rows = []
        for part in range(8):
            base = EMIT_START[part] - WIN_START[part]
            q_count, m_count = Q_BLOCKS[part], M_BLOCKS[part]

            def after(tile):
                q = min(q_count, max(0, -(-tile // Q_COLS)))
                m = min(m_count, max(0, -(-(tile - q_count * Q_COLS) // M_COLS)))
                return q, m

            def before(tile):
                q = min(q_count, max(0, tile // Q_COLS))
                m = min(m_count, max(0, (tile - q_count * Q_COLS) // M_COLS))
                return q, m

            middle = before(base + (K_AG // 2) * N_AG)
            low = (0, 0) if piece == 0 else middle if piece == K_AG // 2 else after(base + piece * N_AG)
            if piece == K_AG - 1:
                high = (q_count, m_count)
            elif piece == K_AG // 2 - 1:
                high = middle
            else:
                high = after(base + (piece + 1) * N_AG)
            rows.append((low[0], high[0], low[1], high[1]))
        table.append(tuple(zip(*rows)))
    return tuple(table)


PIECE_BLOCKS = piece_blocks()


def pick(values, y, x, c):
    total = 0
    for index, value in enumerate(values):
        if value:
            term = value
            for shift, bit in ((2, y), (1, x), (0, c)):
                term = term * (bit if (index >> shift) & 1 else 1 - bit)
            total = total + term
    return total


def step_kernel(gq, go, gu, gd, gn, w_in, m_in, v_in,
                ag, w_out, m_out, v_out, norm_out,
                grads, q_stage, r_ra, r_rb, r_da, r_db, r_pf, r_pa, r_pb,
                r_sa, r_sb, s_sa, s_sb, gsum, mask, state, flat_w, flat_m, flat_v, halo_w, halo_m, halo_v,
                gn_stage, pbuf, nb1, nb2,
                load_sem, store_sem, own_sem, ss, rs_raw, rs_pf, rs_pp, rs_s, rs_h, rs_n1, rs_n2,
                rs_own, rs_pass, rs_own_pair, rs_pair):
    dp = lax.axis_index("dp")
    tp = lax.axis_index("tp")
    y = dp // 4
    x = dp // 2 % 2
    c = dp % 2

    def at(yy, xx, cc):
        return {"dp": yy * 4 + xx * 2 + cc}

    def win(yy, xx, cc):
        return pick(WIN_START, yy, xx, cc)

    ny, nx, nc = 1 - y, 1 - x, 1 - c

    def remote(src, dst, ssem, rsem, dev):
        return pltpu.make_async_remote_copy(
            src_ref=src, dst_ref=dst, send_sem=ssem, recv_sem=rsem, device_id=dev, device_id_type=MESH)

    flats = (flat_w, flat_m, flat_v)
    halos = (halo_w, halo_m, halo_v)
    load_q = pltpu.make_async_copy(gq, q_stage, load_sem.at[0])
    loads = [pltpu.make_async_copy(gn, gn_stage, load_sem.at[1])]
    for index, (src, start, end) in enumerate(((go, O_START, U_START), (gu, U_START, D_START), (gd, D_START, N_START))):
        loads.append(pltpu.make_async_copy(src, grads.at[pl.ds(start, end - start)], load_sem.at[2 + index]))
    state_loads = [pltpu.make_async_copy(src, flats[index], load_sem.at[5 + index])
                   for index, src in enumerate((w_in, m_in, v_in))]
    barrier = pltpu.get_barrier_semaphore()
    load_q.start()
    for copy in loads:
        copy.start()
    for offset in range(1, DP):
        pl.semaphore_signal(barrier, inc=1, device_id={"dp": (dp + offset) % DP}, device_id_type=MESH)
    for offset in range(1, TP):
        pl.semaphore_signal(barrier, inc=1, device_id={"tp": (tp + offset) % TP}, device_id_type=MESH)

    first = (4 - 4 * x) * y

    def turn(k):
        block = (k + first) % 8

        def body(col):
            turned = q_stage[lanes(col), lanes(block)].T
            for index in range(16):
                grads[block * 240 + index * Q_COLS + col] = turned[index * 8:(index + 1) * 8]

        fori(Q_COLS, body)

    load_q.wait()
    fori(4, turn)
    for copy in loads:
        copy.wait()
    for col in range(M_COLS):
        rows = gn_stage[:, col * 128:(col + 1) * 128].astype(F32)
        grads[N_START + col] = jnp.concatenate([rows, jnp.zeros((2, 128), F32)], axis=0).astype(BF16)
    pl.semaphore_wait(barrier, DP + TP - 2)

    def cut(start, k, n=N_RS):
        return pl.ds(start + k * n, n)

    raw_bufs = (r_ra, r_rb, r_da, r_db)

    def raw(stream, cc, k):
        to_y = stream in (0, 2)
        half = 0 if to_y else HALF
        if stream < 2:
            start = win(ny, nx, cc)
        elif to_y:
            start = win(ny, x, cc)
        else:
            start = win(y, nx, cc)
        dev = at(ny, x, cc) if to_y else at(y, nx, cc)
        return remote(grads.at[cut(start + half, k)], raw_bufs[stream].at[c, cut(0, k)],
                      ss.at[S_RAW + 2 * stream + cc], rs_raw.at[stream, k], dev)

    partner = at(y, x, nc)

    def partner_final(k):
        return remote(grads.at[cut(win(y, x, nc), k)], r_pf.at[cut(0, k)], ss.at[S_PF], rs_pf.at[k], partner)

    def partner_relay(which, k):
        if which == 0:
            start, dst = win(y, nx, nc), r_pa
        else:
            start, dst = win(ny, x, nc) + HALF, r_pb
        return remote(grads.at[cut(start, k)], dst.at[cut(0, k)], ss.at[S_PP + which], rs_pp.at[which, k], partner)

    def relayed(which, k):
        src, dst, dev = (s_sa, r_sa, at(y, nx, c)) if which == 0 else (s_sb, r_sb, at(ny, x, c))
        return remote(src.at[cut(0, k)], dst.at[cut(0, k)], ss.at[S_SUM + which], rs_s.at[which, k], dev)

    def halo_copy(index):
        src = (w_in, m_in, v_in)[index]
        return remote(src.at[:, pl.ds(0, HALO * 128)], halos[index],
                      ss.at[S_HALO + index], rs_h.at[index], {"dp": (dp + DP - 1) % DP})

    def arrived(buf, sem):
        pltpu.make_async_copy(buf, buf, sem).wait()

    def sent(buf, sem):
        pltpu.make_async_copy(buf, buf, sem).wait()

    def raw_arrived(stream, k):
        arrived(raw_bufs[stream].at[:, cut(0, k)], rs_raw.at[stream, k])

    def send_diag(*which):
        def step(k):
            for stream, cc in which:
                raw(stream, cc, k).start()
        fori(K_RS, step)

    def send_over_y(k):
        raw(2, 0, k).start()
        raw(2, 1, k).start()
        partner_relay(1, k).start()

    def send_over_x(k):
        raw(3, 0, k).start()
        raw(3, 1, k).start()
        partner_relay(0, k).start()
        partner_final(k).start()
        partner_final(k + K_RS).start()

    @pl.when(y == 0)
    def _():
        send_diag((0, 0), (1, 0), (0, 1), (1, 1))
        fori(K_RS, send_over_y)
        fori(8, turn, 4)
        fori(K_RS, send_over_x)

    @pl.when(y == 1)
    def _():
        send_diag((0, 0), (1, 0), (0, 1))
        turn(4)
        send_diag((1, 1))
        fori(K_RS, send_over_x)
        fori(8, turn, 5)
        fori(K_RS, send_over_y)

    for index in range(3):
        halo_copy(index).start()
    for copy in state_loads:
        copy.start()

    off = PART_ROWS * dp - 8 * win(y, x, c)
    mat_end = MAT_ROWS - 8 * win(y, x, c)
    last = jnp.minimum(off + PART_ROWS, mat_end + jnp.where(tp == 0, 48, 0))
    q_blocks = pick(Q_BLOCKS, y, x, c)
    m_blocks = pick(M_BLOCKS, y, x, c)
    row = lax.broadcasted_iota(jnp.int32, TILE, 0)
    mask[pl.ds(WIN - 5, 5)] = jnp.zeros((5, *TILE), F32)

    def mask_blocks(columns, tile0):
        def body(block):
            for col in range(columns):
                tile = tile0 + block * columns + col
                lane_row = row * columns + (tile0 * 8 + block * columns * 8 + col)
                inside = jnp.logical_and(lane_row >= off, lane_row < last)
                mask[tile] = jnp.where(inside, 1.0, 0.0)
        return body

    fori(q_blocks, mask_blocks(Q_COLS, 0))
    fori(m_blocks, mask_blocks(M_COLS, q_blocks * Q_COLS))

    for copy in state_loads:
        copy.wait()

    def flat_part(k):
        return pl.ds(pl.multiple_of(k * CHUNK, CHUNK), CHUNK)

    def row_part(k):
        return pl.ds(STATE_BASE + k * CHUNK_ROWS, CHUNK_ROWS)

    tail_flat = pl.ds(CHUNKS * CHUNK, TAIL * 128)
    tail_rows = pl.ds(STATE_BASE + CHUNKS * CHUNK_ROWS, TAIL)

    def to_rows(k):
        for index in range(3):
            state[index, row_part(k)] = flats[index][:, flat_part(k)].reshape(CHUNK_ROWS, 128)

    fori(CHUNKS, to_rows)
    for index in range(3):
        state[index, tail_rows] = flats[index][:, tail_flat].reshape(TAIL, 128)

    def relay(which):
        own_start = win(y, nx, c) if which == 0 else win(ny, x, c) + HALF
        raw_buf, pair_buf, out_buf = (r_ra, r_pa, s_sa) if which == 0 else (r_rb, r_pb, s_sb)

        def body(k):
            raw_arrived(which, k)
            arrived(pair_buf.at[cut(0, k)], rs_pp.at[which, k])

            def tiles(index):
                here = pl.ds(k * N_RS + index * STEP_TILES, STEP_TILES)
                total = grads[pl.ds(own_start + k * N_RS + index * STEP_TILES, STEP_TILES)].astype(F32)
                total = total + pair_buf[here].astype(F32)
                total = total + raw_buf[0, here].astype(F32)
                total = total + raw_buf[1, here].astype(F32)
                out_buf[here] = total

            fori(N_RS // STEP_TILES, tiles)
            relayed(which, k).start()
        return body

    relay_a, relay_b = relay(0), relay(1)

    def relay_step(k):
        relay_a(k)
        relay_b(k)

    fori(K_RS, relay_step)

    for index in range(3):
        arrived(halos[index], rs_h.at[index])
        state[index, pl.ds(STATE_BASE + PART_ROWS, HALO)] = halos[index][...].reshape(HALO, 128)

    def finish(which):
        half = 0 if which == 0 else HALF
        raw_buf, sum_buf = (r_da, r_sa) if which == 0 else (r_db, r_sb)

        def body(k, acc):
            raw_arrived(2 + which, k)
            arrived(r_pf.at[cut(half, k)], rs_pf.at[k + which * K_RS])
            arrived(sum_buf.at[cut(0, k)], rs_s.at[which, k])

            def tiles(index, acc):
                here = pl.ds(k * N_RS + index * STEP_TILES, STEP_TILES)
                part = pl.ds(half + k * N_RS + index * STEP_TILES, STEP_TILES)
                total = grads[pl.ds(win(y, x, c) + half + k * N_RS + index * STEP_TILES, STEP_TILES)].astype(F32)
                total = total + r_pf[part].astype(F32)
                total = total + raw_buf[0, here].astype(F32)
                total = total + raw_buf[1, here].astype(F32)
                total = (total + sum_buf[here]) * 0.125
                gsum[part] = total
                square = jnp.where(mask[part] > 0.5, total * total, 0.0)
                return acc + jnp.sum(square, axis=0)

            return lax.fori_loop(0, N_RS // STEP_TILES, tiles, acc)
        return body

    finish_a, finish_b = finish(0), finish(1)
    acc = lax.fori_loop(0, K_RS, lambda k, acc: finish_b(k, finish_a(k, acc)), jnp.zeros(TILE, F32))

    nb1[dp] = acc

    for offset in range(1, DP):
        remote(nb1.at[dp], nb1.at[dp], ss.at[S_N1], rs_n1, {"dp": (dp + offset) % DP}).start()
    arrived(nb1.at[pl.ds(0, DP - 1)], rs_n1)
    plane = nb1[0]
    for index in range(1, DP):
        plane = plane + nb1[index]
    nb2[tp] = plane
    for offset in range(1, TP):
        remote(nb2.at[tp], nb2.at[tp], ss.at[S_N2], rs_n2, {"tp": (tp + offset) % TP}).start()
    arrived(nb2.at[pl.ds(0, TP - 1)], rs_n2)
    total = nb2[0] + nb2[1] + nb2[2] + nb2[3]
    total = jnp.sum(jnp.sum(total, axis=0, keepdims=True), axis=1, keepdims=True)
    norm = jnp.sqrt(jnp.broadcast_to(total, TILE))
    norm_out[...] = norm
    clip = jnp.minimum(1.0, MAX_NORM / (norm + NORM_EPS))

    def update_blocks(columns, tile0):
        def body(block):
            row0 = tile0 * 8 + block * columns * 8
            decay = jnp.where(row0 < mat_end, DECAY, 0.0)
            for col in range(columns):
                tile = tile0 + block * columns + col
                here = pl.ds(STATE_BASE - off + row0 + col, 8, stride=columns)
                grad = gsum[tile] * clip
                w_old = state[0, here]
                m_new = BETA_ONE * state[1, here] + (1.0 - BETA_ONE) * grad
                v_new = BETA_TWO * state[2, here] + (1.0 - BETA_TWO) * grad * grad
                step_dir = (m_new * (1.0 / BIAS_ONE)) / (jnp.sqrt(v_new * (1.0 / BIAS_TWO)) + ADAM_EPS)
                w_new = w_old - LEARN_RATE * (step_dir + decay * w_old)
                state[0, here] = w_new
                state[1, here] = m_new
                state[2, here] = v_new
                pbuf[tile] = w_new.astype(BF16)
        return body

    update_q = update_blocks(Q_COLS, 0)
    update_m = update_blocks(M_COLS, q_blocks * Q_COLS)

    emit0 = pick([e - s for e, s in zip(EMIT_START, WIN_START)], y, x, c)

    def piece(k):
        return pl.ds(k * N_AG, N_AG)

    part_x, part_y, part_d = y * 4 + nx * 2 + c, ny * 4 + x * 2 + c, ny * 4 + nx * 2 + c
    dev_x, dev_y = at(y, nx, c), at(ny, x, c)

    def own_out(which, k):
        dev = (dev_x, dev_y, partner)[which]
        rsem = rs_own_pair if which == 2 else rs_own.at[which, k]
        return remote(pbuf.at[pl.ds(emit0 + k * N_AG, N_AG)], ag.at[dp, piece(k)], ss.at[S_OWN + which], rsem, dev)

    def pass_out(which, k):
        part, dev = ((part_x, dev_y), (part_y, dev_x))[which]
        return remote(ag.at[part, piece(k)], ag.at[part, piece(k)], ss.at[S_PASS], rs_pass.at[k], dev)

    def pair_out(which, k):
        part = (part_x, part_y, part_d)[which]
        return remote(ag.at[part, piece(k)], ag.at[part, piece(k)], ss.at[S_PAIR + which], rs_pair.at[which], partner)

    own_copy = pltpu.make_async_copy(pbuf.at[pl.ds(emit0, EMIT)], ag.at[dp], own_sem)

    for k, bounds in enumerate(PIECE_BLOCKS):
        q_from, q_to, m_from, m_to = (pick(bound, y, x, c) for bound in bounds)
        fori(q_to, update_q, q_from)
        fori(m_to, update_m, m_from)
        own_out(k % 2, PIECE_ORDER[k]).start()
        own_out(2, PIECE_ORDER[k]).start()

    def send_rest(k):
        own_out(0, HALF_AG + k).start()
        own_out(1, k).start()

    fori(HALF_AG, send_rest)
    own_copy.start()

    def to_flat(k):
        for index in range(3):
            flats[index][:, flat_part(k)] = state[index, row_part(k)].reshape(1, CHUNK)

    fori(CHUNKS, to_flat)
    stores = []
    for index, dst in enumerate((w_out, m_out, v_out)):
        flats[index][:, tail_flat] = state[index, tail_rows].reshape(1, TAIL * 128)
        stores.append(pltpu.make_async_copy(flats[index], dst, store_sem.at[index]))
        stores[-1].start()

    def first_half(k):
        arrived(ag.at[part_x, piece(k)], rs_own.at[0, k])
        pass_out(0, k).start()
        pair_out(0, k).start()
        later = k + HALF_AG
        arrived(ag.at[part_y, piece(later)], rs_own.at[1, later])
        pass_out(1, later).start()
        pair_out(1, later).start()

    def second_half(k):
        later = k + HALF_AG
        arrived(ag.at[part_x, piece(later)], rs_own.at[0, later])
        pair_out(0, later).start()
        arrived(ag.at[part_y, piece(k)], rs_own.at[1, k])
        pair_out(1, k).start()

    def diagonal(k):
        for index in (k, k + HALF_AG):
            arrived(ag.at[part_d, piece(index)], rs_pass.at[index])
            pair_out(2, index).start()

    fori(HALF_AG, first_half)
    fori(HALF_AG, second_half)
    fori(HALF_AG, diagonal)

    for stream in range(4):
        for cc in range(2):
            sent(raw_bufs[stream].at[0], ss.at[S_RAW + 2 * stream + cc])
    sent(r_pf, ss.at[S_PF])
    for which in range(2):
        sent(r_pa, ss.at[S_PP + which])
        sent(s_sa, ss.at[S_SUM + which])
    for which in range(3):
        sent(halos[which], ss.at[S_HALO + which])
        sent(ag.at[0], ss.at[S_OWN + which])
        sent(ag.at[0], ss.at[S_PAIR + which])
    sent(nb1.at[pl.ds(0, DP - 1)], ss.at[S_N1])
    sent(nb2.at[pl.ds(0, TP - 1)], ss.at[S_N2])
    sent(ag.at[0], ss.at[S_PASS])
    arrived(ag.at[y * 4 + x * 2 + nc], rs_own_pair)
    for which, part in enumerate((y * 4 + nx * 2 + nc, ny * 4 + x * 2 + nc, ny * 4 + nx * 2 + nc)):
        arrived(ag.at[part], rs_pair.at[which])
    own_copy.wait()
    for copy in stores:
        copy.wait()


def pieces_of(start, end):
    found = []
    for part in range(DP):
        low, high = max(start, EMIT_START[part]), min(end, EMIT_END[part])
        if low < high:
            found.append((part, low - EMIT_START[part], low - start, high - low))
    return found


def lay_out_kernel(ag, w_in, m_in, v_in, norm, q_out, o_out, u_out, d_out, n_out, w_out, m_out, v_out, norm_out,
                   tiles, n_tiles, q_stage, flat_w, flat_m, flat_v, in_sem, out_sem, q_sem, flat_sem):
    flats = (flat_w, flat_m, flat_v)

    def ranges(dst, start, end, sem, base):
        return [pltpu.make_async_copy(ag.at[part, pl.ds(low, count)], dst.at[pl.ds(offset, count)], sem.at[base + index])
                for index, (part, low, offset, count) in enumerate(pieces_of(start, end))]

    loads = ranges(tiles, 0, O_START, in_sem, 0)
    loads += ranges(n_tiles, N_START, TILES, in_sem, len(loads))
    outs = []
    for dst, start, end in ((o_out, O_START, U_START), (u_out, U_START, D_START), (d_out, D_START, N_START)):
        outs += ranges(dst, start, end, out_sem, len(outs))
    flat_loads = [pltpu.make_async_copy(src, flats[index], flat_sem.at[index])
                  for index, src in enumerate((w_in, m_in, v_in))]
    flat_stores = [pltpu.make_async_copy(flats[index], dst, flat_sem.at[3 + index])
                   for index, dst in enumerate((w_out, m_out, v_out))]

    def q_store(block):
        return pltpu.make_async_copy(q_stage.at[:, lanes(block)], q_out.at[:, lanes(block)], q_sem.at[block])

    def turn(block):
        def body(col):
            part = jnp.concatenate([tiles[block * 240 + index * Q_COLS + col] for index in range(16)], axis=0)
            q_stage[lanes(col), lanes(block)] = part.T

        fori(Q_COLS, body)
        q_store(block).start()

    for copy in loads + flat_loads + outs:
        copy.start()
    norm_out[0, 0] = jnp.max(norm[...])
    loads[0].wait()
    fori(2, turn)
    loads[1].wait()
    fori(4, turn, 2)
    for index in range(3):
        flat_loads[index].wait()
        flat_stores[index].start()
    for copy in loads[2:]:
        copy.wait()
    fori(8, turn, 4)
    for col in range(M_COLS):
        n_out[:, col * 128:(col + 1) * 128] = n_tiles[col].astype(F32)[:6].astype(BF16)
    for copy in outs + flat_stores:
        copy.wait()
    fori(8, lambda block: q_store(block).wait())


def to_tiles(matrix):
    rows, cols = matrix.shape
    return matrix.reshape(rows // 8, 8, cols // 128, 128).transpose(0, 2, 1, 3).reshape(rows * cols // 1024, 8, 128)


def from_tiles(tiles, rows, cols):
    return tiles.reshape(rows // 8, cols // 128, 8, 128).transpose(0, 2, 1, 3).reshape(rows, cols)


on_chip = pltpu.with_memory_space_constraint


def in_hbm(*arrays):
    return [on_chip(array, pltpu.HBM) for array in arrays]


def any_spec(count):
    return [pl.BlockSpec(memory_space=pltpu.HBM)] * count


def solution(mesh):
    dma = pltpu.SemaphoreType.DMA

    q_shape = (1920, 1024)
    params = functools.partial(pltpu.CompilerParams, vmem_limit_bytes=VMEM_LIMIT)

    def local_step(g_qkv, g_out, g_up, g_down, g_norms, master, mom_one, mom_two):
        gq = g_qkv[0].transpose(1, 2, 3, 0).reshape(q_shape)
        go, gu, gd = to_tiles(g_out[0]), to_tiles(g_up[0]), to_tiles(g_down[0])
        gn = g_norms[0]
        part = jax.ShapeDtypeStruct(master.shape, F32)
        flat = pltpu.VMEM((1, FLAT), F32)
        tile_count = (U_START - O_START, D_START - U_START, N_START - D_START)
        win_f32, half_f32 = pltpu.VMEM((WIN, *TILE), F32), pltpu.VMEM((HALF, *TILE), F32)
        half_bf16 = pltpu.VMEM((HALF, *TILE), BF16)
        scratch = [
            pltpu.VMEM((TILES, *TILE), BF16),
            pltpu.VMEM(q_shape, BF16),
            *[pltpu.VMEM((2, HALF, *TILE), BF16)] * 4,
            pltpu.VMEM((WIN, *TILE), BF16),
            half_bf16, half_bf16, half_f32, half_f32, half_f32, half_f32, win_f32, win_f32,
            pltpu.VMEM((3, STATE_ROWS, 128), F32),
            flat, flat, flat,
            *[pltpu.VMEM((1, HALO * 128), F32)] * 3,
            pltpu.VMEM(g_norms.shape[1:], BF16),
            pltpu.VMEM((WIN + 16, *TILE), BF16),
            pltpu.VMEM((DP, *TILE), F32),
            pltpu.VMEM((TP, *TILE), F32),
            dma((8,)), dma((3,)), dma(()), dma((SENDS,)),
            dma((4, K_RS)), dma((2 * K_RS,)), dma((2, K_RS)), dma((2, K_RS)), dma((3,)), dma(()), dma(()),
            dma((2, K_AG)), dma((K_AG,)), dma(()), dma((3,)),
        ]
        ag, w_new, m_new, v_new, norm = pl.pallas_call(
            step_kernel,
            name="reduce_update_gather",
            out_shape=[pltpu.VMEM((DP, EMIT, *TILE), BF16), part, part, part,
                       pltpu.VMEM(TILE, F32)],
            in_specs=any_spec(8),
            out_specs=[pl.BlockSpec(memory_space=pl.ANY)] + any_spec(3) + [pl.BlockSpec(memory_space=pltpu.VMEM)],
            scratch_shapes=scratch,
            compiler_params=params(collective_id=0, has_side_effects=True, vmem_limit_bytes=STEP_VMEM),
        )(*in_hbm(gq, go, gu, gd, gn, master, mom_one, mom_two))
        pq, po, pu, pd, pn, w_new, m_new, v_new, norm = pl.pallas_call(
            lay_out_kernel,
            name="lay_out",
            out_shape=[jax.ShapeDtypeStruct(q_shape, BF16),
                       *[jax.ShapeDtypeStruct((count, *TILE), BF16) for count in tile_count],
                       jax.ShapeDtypeStruct(g_norms.shape[1:], BF16), part, part, part, jax.ShapeDtypeStruct((1, 1), F32)],
            in_specs=[pl.BlockSpec(memory_space=pl.ANY)] + any_spec(3) + [pl.BlockSpec(memory_space=pltpu.VMEM)],
            out_specs=any_spec(4) + [pl.BlockSpec(memory_space=pltpu.VMEM)] + any_spec(3)
            + [pl.BlockSpec(memory_space=pltpu.SMEM)],
            scratch_shapes=[pltpu.VMEM((O_START, *TILE), BF16), pltpu.VMEM((M_COLS, *TILE), BF16),
                            pltpu.VMEM(q_shape, BF16), flat, flat, flat, dma((8,)), dma((12,)), dma((8,)), dma((6,))],
            compiler_params=params(),
        )(on_chip(ag, pltpu.VMEM), *in_hbm(w_new, m_new, v_new), on_chip(norm, pltpu.VMEM))
        p_qkv = pq.reshape(8, 3, 80, 1024).transpose(3, 0, 1, 2)
        return (p_qkv, *[from_tiles(tiles, tiles.shape[0], 1024) for tiles in (po, pu, pd)],
                pn, w_new, m_new, v_new, norm[0, 0])

    return jax.shard_map(local_step, mesh=mesh, in_specs=ARG_SPECS, out_specs=OUT_SPECS, check_vma=False)
```

```python
import functools

import jax
import jax.numpy as jnp
from jax import lax
from jax.experimental import pallas as pl
from jax.experimental.pallas import tpu as pltpu
from jax.sharding import PartitionSpec as P

STEP = 20
BETA_ONE = 0.9
BETA_TWO = 0.95
ADAM_EPS = 1e-8
DECAY = 0.1
LEARN_RATE = 1e-4
MAX_NORM = 1.0
NORM_EPS = 1e-6
BIAS_ONE = 1.0 - BETA_ONE ** STEP
BIAS_TWO = 1.0 - BETA_TWO ** STEP
TP_COL = P(None, "tp")
ROW_DP = P("dp")
STATE = P("tp", "dp")
ARG_SPECS = (P("dp", None, "tp"), P("dp", "tp"), P("dp", None, "tp"), P("dp", "tp"), ROW_DP, STATE, STATE, STATE)
OUT_SPECS = (TP_COL, P("tp"), TP_COL, P("tp"), P(), STATE, STATE, STATE, P())

MESH = pl.DeviceIdType.MESH
F32 = jnp.float32
BF16 = jnp.bfloat16

Q_TILES = 1920
TILES = 4616
Q_COLS = 15
M_COLS = 8
PART_ROWS = 4614
MAT_ROWS = 36864
WIN = 600
HALF = WIN // 2
WIN_START = (0, 570, 1140, 1725, 2304, 2880, 3456, 4016)
EMIT_START = (0, 585, 1155, 1740, 2312, 2888, 3464, 4040)
EMIT_END = (585, 1155, 1740, 2312, 2888, 3464, 4040, 4616)
Q_BLOCKS = (40, 40, 40, 13, 0, 0, 0, 0)
M_BLOCKS = (0, 0, 0, 50, 75, 75, 75, 75)
EMIT = 588
STATE_BASE = 176
STATE_ROWS = 4984
HALO = 80

K_RS = 5
N_RS = HALF // K_RS
K_AG = 12
N_AG = EMIT // K_AG
STEP_TILES = 4
HALF_AG = K_AG // 2
FLAT = PART_ROWS * 128
CHUNK_ROWS = 64
CHUNK = CHUNK_ROWS * 128
CHUNKS = PART_ROWS // CHUNK_ROWS
TAIL = PART_ROWS - CHUNKS * CHUNK_ROWS
TILE = (8, 128)
TURN_UNROLL = 5
VMEM_LIMIT = 43 * 1024 * 1024
STEP_VMEM = 43 * 1024 * 1024
DP, TP = 8, 4
O_START, U_START, D_START, N_START = 1920, 2560, 3584, 4608
S_RAW, S_PF, S_PP, S_SUM, S_HALO, S_N1, S_N2, S_OWN, S_PAIR, S_PASS, SENDS = 0, 8, 9, 11, 13, 16, 17, 18, 21, 24, 25


def fori(count, step, start=0):
    def body(k, carry):
        step(k)
        return carry

    lax.fori_loop(start, count, body, 0)


def lanes(block):
    return pl.ds(pl.multiple_of(block * 128, 128), 128)


PIECE_ORDER = tuple(k // 2 + (K_AG // 2) * (k % 2) for k in range(K_AG))


def piece_blocks():
    table = []
    for k, piece in enumerate(PIECE_ORDER):
        rows = []
        for part in range(8):
            base = EMIT_START[part] - WIN_START[part]
            q_count, m_count = Q_BLOCKS[part], M_BLOCKS[part]

            def after(tile):
                q = min(q_count, max(0, -(-tile // Q_COLS)))
                m = min(m_count, max(0, -(-(tile - q_count * Q_COLS) // M_COLS)))
                return q, m

            def before(tile):
                q = min(q_count, max(0, tile // Q_COLS))
                m = min(m_count, max(0, (tile - q_count * Q_COLS) // M_COLS))
                return q, m

            middle = before(base + (K_AG // 2) * N_AG)
            low = (0, 0) if piece == 0 else middle if piece == K_AG // 2 else after(base + piece * N_AG)
            if piece == K_AG - 1:
                high = (q_count, m_count)
            elif piece == K_AG // 2 - 1:
                high = middle
            else:
                high = after(base + (piece + 1) * N_AG)
            rows.append((low[0], high[0], low[1], high[1]))
        table.append(tuple(zip(*rows)))
    return tuple(table)


PIECE_BLOCKS = piece_blocks()


def pick(values, y, x, c):
    total = 0
    for index, value in enumerate(values):
        if value:
            term = value
            for shift, bit in ((2, y), (1, x), (0, c)):
                term = term * (bit if (index >> shift) & 1 else 1 - bit)
            total = total + term
    return total


def step_kernel(gq, go, gu, gd, gn, w_in, m_in, v_in,
                ag, w_out, m_out, v_out, norm_out,
                grads, q_stage, r_ra, r_rb, r_da, r_db, r_pf, r_pa, r_pb,
                r_sa, r_sb, s_sa, s_sb, gsum, mask, state, flat_buf, halo_w, halo_m, halo_v,
                gn_stage, pbuf, nb1, nb2,
                load_sem, store_sem, own_sem, ss, rs_raw, rs_pf, rs_pp, rs_s, rs_h, rs_n1, rs_n2,
                rs_own, rs_pass, rs_own_pair, rs_pair):
    dp = lax.axis_index("dp")
    tp = lax.axis_index("tp")
    y = dp // 4
    x = dp // 2 % 2
    c = dp % 2

    def at(yy, xx, cc):
        return {"dp": yy * 4 + xx * 2 + cc}

    def win(yy, xx, cc):
        return pick(WIN_START, yy, xx, cc)

    ny, nx, nc = 1 - y, 1 - x, 1 - c

    def remote(src, dst, ssem, rsem, dev):
        return pltpu.make_async_remote_copy(
            src_ref=src, dst_ref=dst, send_sem=ssem, recv_sem=rsem, device_id=dev, device_id_type=MESH)

    halos = (halo_w, halo_m, halo_v)
    load_q = pltpu.make_async_copy(gq, q_stage, load_sem.at[0])
    loads = [pltpu.make_async_copy(gn, gn_stage, load_sem.at[1])]
    for index, (src, start, end) in enumerate(((go, O_START, U_START), (gu, U_START, D_START), (gd, D_START, N_START))):
        loads.append(pltpu.make_async_copy(src, grads.at[pl.ds(start, end - start)], load_sem.at[2 + index]))
    state_loads = [pltpu.make_async_copy(src, flat_buf, load_sem.at[5 + index])
                   for index, src in enumerate((w_in, m_in, v_in))]
    barrier = pltpu.get_barrier_semaphore()
    load_q.start()
    for copy in loads:
        copy.start()
    for offset in range(1, DP):
        pl.semaphore_signal(barrier, inc=1, device_id={"dp": (dp + offset) % DP}, device_id_type=MESH)
    for offset in range(1, TP):
        pl.semaphore_signal(barrier, inc=1, device_id={"tp": (tp + offset) % TP}, device_id_type=MESH)

    first = (4 - 4 * x) * y

    def turn(k):
        block = (k + first) % 8

        def body(col):
            turned = q_stage[lanes(col), lanes(block)].T
            for index in range(16):
                grads[block * 240 + index * Q_COLS + col] = turned[index * 8:(index + 1) * 8]

        fori(Q_COLS, body)

    load_q.wait()
    fori(4, turn)
    for copy in loads:
        copy.wait()
    for col in range(M_COLS):
        rows = gn_stage[:, col * 128:(col + 1) * 128].astype(F32)
        grads[N_START + col] = jnp.concatenate([rows, jnp.zeros((2, 128), F32)], axis=0).astype(BF16)
    pl.semaphore_wait(barrier, DP + TP - 2)

    def cut(start, k, n=N_RS):
        return pl.ds(start + k * n, n)

    raw_bufs = (r_ra, r_rb, r_da, r_db)

    def raw(stream, cc, k):
        to_y = stream in (0, 2)
        half = 0 if to_y else HALF
        if stream < 2:
            start = win(ny, nx, cc)
        elif to_y:
            start = win(ny, x, cc)
        else:
            start = win(y, nx, cc)
        dev = at(ny, x, cc) if to_y else at(y, nx, cc)
        return remote(grads.at[cut(start + half, k)], raw_bufs[stream].at[c, cut(0, k)],
                      ss.at[S_RAW + 2 * stream + cc], rs_raw.at[stream, k], dev)

    partner = at(y, x, nc)

    def partner_final(k):
        return remote(grads.at[cut(win(y, x, nc), k)], r_pf.at[cut(0, k)], ss.at[S_PF], rs_pf.at[k], partner)

    def partner_relay(which, k):
        if which == 0:
            start, dst = win(y, nx, nc), r_pa
        else:
            start, dst = win(ny, x, nc) + HALF, r_pb
        return remote(grads.at[cut(start, k)], dst.at[cut(0, k)], ss.at[S_PP + which], rs_pp.at[which, k], partner)

    def relayed(which, k):
        src, dst, dev = (s_sa, r_sa, at(y, nx, c)) if which == 0 else (s_sb, r_sb, at(ny, x, c))
        return remote(src.at[cut(0, k)], dst.at[cut(0, k)], ss.at[S_SUM + which], rs_s.at[which, k], dev)

    def halo_copy(index):
        src = (w_in, m_in, v_in)[index]
        return remote(src.at[:, pl.ds(0, HALO * 128)], halos[index],
                      ss.at[S_HALO + index], rs_h.at[index], {"dp": (dp + DP - 1) % DP})

    def arrived(buf, sem):
        pltpu.make_async_copy(buf, buf, sem).wait()

    def sent(buf, sem):
        pltpu.make_async_copy(buf, buf, sem).wait()

    def raw_arrived(stream, k):
        arrived(raw_bufs[stream].at[:, cut(0, k)], rs_raw.at[stream, k])

    def send_diag(*which):
        def step(k):
            for stream, cc in which:
                raw(stream, cc, k).start()
        fori(K_RS, step)

    def send_over_y(k):
        raw(2, 0, k).start()
        raw(2, 1, k).start()
        partner_relay(1, k).start()

    def send_over_x(k):
        raw(3, 0, k).start()
        raw(3, 1, k).start()
        partner_relay(0, k).start()
        partner_final(k).start()
        partner_final(k + K_RS).start()

    @pl.when(y == 0)
    def _():
        send_diag((0, 0), (1, 0), (0, 1), (1, 1))
        fori(K_RS, send_over_y)
        fori(8, turn, 4)
        fori(K_RS, send_over_x)

    @pl.when(y == 1)
    def _():
        send_diag((0, 0), (1, 0), (0, 1))
        turn(4)
        send_diag((1, 1))
        fori(K_RS, send_over_x)
        fori(8, turn, 5)
        fori(K_RS, send_over_y)

    for index in range(3):
        halo_copy(index).start()
    state_loads[0].start()

    off = PART_ROWS * dp - 8 * win(y, x, c)
    mat_end = MAT_ROWS - 8 * win(y, x, c)
    last = jnp.minimum(off + PART_ROWS, mat_end + jnp.where(tp == 0, 48, 0))
    q_blocks = pick(Q_BLOCKS, y, x, c)
    m_blocks = pick(M_BLOCKS, y, x, c)
    row = lax.broadcasted_iota(jnp.int32, TILE, 0)
    mask[pl.ds(WIN - 5, 5)] = jnp.zeros((5, *TILE), F32)

    def mask_blocks(columns, tile0):
        def body(block):
            for col in range(columns):
                tile = tile0 + block * columns + col
                lane_row = row * columns + (tile0 * 8 + block * columns * 8 + col)
                inside = jnp.logical_and(lane_row >= off, lane_row < last)
                mask[tile] = jnp.where(inside, 1.0, 0.0)
        return body

    fori(q_blocks, mask_blocks(Q_COLS, 0))
    fori(m_blocks, mask_blocks(M_COLS, q_blocks * Q_COLS))

    def flat_part(k):
        return pl.ds(pl.multiple_of(k * CHUNK, CHUNK), CHUNK)

    def row_part(k):
        return pl.ds(STATE_BASE + k * CHUNK_ROWS, CHUNK_ROWS)

    tail_flat = pl.ds(CHUNKS * CHUNK, TAIL * 128)
    tail_rows = pl.ds(STATE_BASE + CHUNKS * CHUNK_ROWS, TAIL)

    for index in range(3):
        def to_rows(k):
            state[index, row_part(k)] = flat_buf[:, flat_part(k)].reshape(CHUNK_ROWS, 128)

        state_loads[index].wait()
        fori(CHUNKS, to_rows)
        state[index, tail_rows] = flat_buf[:, tail_flat].reshape(TAIL, 128)
        if index < 2:
            state_loads[index + 1].start()

    def relay(which):
        own_start = win(y, nx, c) if which == 0 else win(ny, x, c) + HALF
        raw_buf, pair_buf, out_buf = (r_ra, r_pa, s_sa) if which == 0 else (r_rb, r_pb, s_sb)

        def body(k):
            raw_arrived(which, k)
            arrived(pair_buf.at[cut(0, k)], rs_pp.at[which, k])

            def tiles(index):
                here = pl.ds(k * N_RS + index * STEP_TILES, STEP_TILES)
                total = grads[pl.ds(own_start + k * N_RS + index * STEP_TILES, STEP_TILES)].astype(F32)
                total = total + pair_buf[here].astype(F32)
                total = total + raw_buf[0, here].astype(F32)
                total = total + raw_buf[1, here].astype(F32)
                out_buf[here] = total

            fori(N_RS // STEP_TILES, tiles)
            relayed(which, k).start()
        return body

    relay_a, relay_b = relay(0), relay(1)

    def relay_step(k):
        relay_a(k)
        relay_b(k)

    fori(K_RS, relay_step)

    for index in range(3):
        arrived(halos[index], rs_h.at[index])
        state[index, pl.ds(STATE_BASE + PART_ROWS, HALO)] = halos[index][...].reshape(HALO, 128)

    def finish(which):
        half = 0 if which == 0 else HALF
        raw_buf, sum_buf = (r_da, r_sa) if which == 0 else (r_db, r_sb)

        def body(k, acc):
            raw_arrived(2 + which, k)
            arrived(r_pf.at[cut(half, k)], rs_pf.at[k + which * K_RS])
            arrived(sum_buf.at[cut(0, k)], rs_s.at[which, k])

            def tiles(index, acc):
                here = pl.ds(k * N_RS + index * STEP_TILES, STEP_TILES)
                part = pl.ds(half + k * N_RS + index * STEP_TILES, STEP_TILES)
                total = grads[pl.ds(win(y, x, c) + half + k * N_RS + index * STEP_TILES, STEP_TILES)].astype(F32)
                total = total + r_pf[part].astype(F32)
                total = total + raw_buf[0, here].astype(F32)
                total = total + raw_buf[1, here].astype(F32)
                total = (total + sum_buf[here]) * 0.125
                gsum[part] = total
                square = jnp.where(mask[part] > 0.5, total * total, 0.0)
                return acc + jnp.sum(square, axis=0)

            return lax.fori_loop(0, N_RS // STEP_TILES, tiles, acc)
        return body

    finish_a, finish_b = finish(0), finish(1)
    acc = lax.fori_loop(0, K_RS, lambda k, acc: finish_b(k, finish_a(k, acc)), jnp.zeros(TILE, F32))

    nb1[dp] = acc

    for offset in range(1, DP):
        remote(nb1.at[dp], nb1.at[dp], ss.at[S_N1], rs_n1, {"dp": (dp + offset) % DP}).start()
    arrived(nb1.at[pl.ds(0, DP - 1)], rs_n1)
    plane = nb1[0]
    for index in range(1, DP):
        plane = plane + nb1[index]
    nb2[tp] = plane
    for offset in range(1, TP):
        remote(nb2.at[tp], nb2.at[tp], ss.at[S_N2], rs_n2, {"tp": (tp + offset) % TP}).start()
    arrived(nb2.at[pl.ds(0, TP - 1)], rs_n2)
    total = nb2[0] + nb2[1] + nb2[2] + nb2[3]
    total = jnp.sum(jnp.sum(total, axis=0, keepdims=True), axis=1, keepdims=True)
    norm = jnp.sqrt(jnp.broadcast_to(total, TILE))
    norm_out[...] = norm
    clip = jnp.minimum(1.0, MAX_NORM / (norm + NORM_EPS))

    def update_blocks(columns, tile0):
        def body(block):
            row0 = tile0 * 8 + block * columns * 8
            decay = jnp.where(row0 < mat_end, DECAY, 0.0)
            for col in range(columns):
                tile = tile0 + block * columns + col
                here = pl.ds(STATE_BASE - off + row0 + col, 8, stride=columns)
                grad = gsum[tile] * clip
                w_old = state[0, here]
                m_new = BETA_ONE * state[1, here] + (1.0 - BETA_ONE) * grad
                v_new = BETA_TWO * state[2, here] + (1.0 - BETA_TWO) * grad * grad
                step_dir = (m_new * (1.0 / BIAS_ONE)) / (jnp.sqrt(v_new * (1.0 / BIAS_TWO)) + ADAM_EPS)
                w_new = w_old - LEARN_RATE * (step_dir + decay * w_old)
                state[0, here] = w_new
                state[1, here] = m_new
                state[2, here] = v_new
                pbuf[tile] = w_new.astype(BF16)
        return body

    update_q = update_blocks(Q_COLS, 0)
    update_m = update_blocks(M_COLS, q_blocks * Q_COLS)

    emit0 = pick([e - s for e, s in zip(EMIT_START, WIN_START)], y, x, c)

    def piece(k):
        return pl.ds(k * N_AG, N_AG)

    part_x, part_y, part_d = y * 4 + nx * 2 + c, ny * 4 + x * 2 + c, ny * 4 + nx * 2 + c
    dev_x, dev_y = at(y, nx, c), at(ny, x, c)

    def own_out(which, k):
        dev = (dev_x, dev_y, partner)[which]
        rsem = rs_own_pair if which == 2 else rs_own.at[which, k]
        return remote(pbuf.at[pl.ds(emit0 + k * N_AG, N_AG)], ag.at[dp, piece(k)], ss.at[S_OWN + which], rsem, dev)

    def pass_out(which, k):
        part, dev = ((part_x, dev_y), (part_y, dev_x))[which]
        return remote(ag.at[part, piece(k)], ag.at[part, piece(k)], ss.at[S_PASS], rs_pass.at[k], dev)

    def pair_out(which, k):
        part = (part_x, part_y, part_d)[which]
        return remote(ag.at[part, piece(k)], ag.at[part, piece(k)], ss.at[S_PAIR + which], rs_pair.at[which], partner)

    own_copy = pltpu.make_async_copy(pbuf.at[pl.ds(emit0, EMIT)], ag.at[dp], own_sem)

    for k, bounds in enumerate(PIECE_BLOCKS):
        q_from, q_to, m_from, m_to = (pick(bound, y, x, c) for bound in bounds)
        fori(q_to, update_q, q_from)
        fori(m_to, update_m, m_from)
        own_out(k % 2, PIECE_ORDER[k]).start()
        own_out(2, PIECE_ORDER[k]).start()

    def send_rest(k):
        own_out(0, HALF_AG + k).start()
        own_out(1, k).start()

    fori(HALF_AG, send_rest)
    own_copy.start()

    def store_state(index):
        def to_flat(k):
            flat_buf[:, flat_part(k)] = state[index, row_part(k)].reshape(1, CHUNK)

        fori(CHUNKS, to_flat)
        flat_buf[:, tail_flat] = state[index, tail_rows].reshape(1, TAIL * 128)
        copy = pltpu.make_async_copy(flat_buf, (w_out, m_out, v_out)[index], store_sem.at[index])
        copy.start()
        return copy

    def first_half(k):
        arrived(ag.at[part_x, piece(k)], rs_own.at[0, k])
        pass_out(0, k).start()
        pair_out(0, k).start()
        later = k + HALF_AG
        arrived(ag.at[part_y, piece(later)], rs_own.at[1, later])
        pass_out(1, later).start()
        pair_out(1, later).start()

    def second_half(k):
        later = k + HALF_AG
        arrived(ag.at[part_x, piece(later)], rs_own.at[0, later])
        pair_out(0, later).start()
        arrived(ag.at[part_y, piece(k)], rs_own.at[1, k])
        pair_out(1, k).start()

    def diagonal(k):
        for index in (k, k + HALF_AG):
            arrived(ag.at[part_d, piece(index)], rs_pass.at[index])
            pair_out(2, index).start()

    for index, step in enumerate((first_half, second_half, diagonal)):
        store = store_state(index)
        fori(HALF_AG, step)
        store.wait()

    for stream in range(4):
        for cc in range(2):
            sent(raw_bufs[stream].at[0], ss.at[S_RAW + 2 * stream + cc])
    sent(r_pf, ss.at[S_PF])
    for which in range(2):
        sent(r_pa, ss.at[S_PP + which])
        sent(s_sa, ss.at[S_SUM + which])
    for which in range(3):
        sent(halos[which], ss.at[S_HALO + which])
        sent(ag.at[0], ss.at[S_OWN + which])
        sent(ag.at[0], ss.at[S_PAIR + which])
    sent(nb1.at[pl.ds(0, DP - 1)], ss.at[S_N1])
    sent(nb2.at[pl.ds(0, TP - 1)], ss.at[S_N2])
    sent(ag.at[0], ss.at[S_PASS])
    arrived(ag.at[y * 4 + x * 2 + nc], rs_own_pair)
    for which, part in enumerate((y * 4 + nx * 2 + nc, ny * 4 + x * 2 + nc, ny * 4 + nx * 2 + nc)):
        arrived(ag.at[part], rs_pair.at[which])
    own_copy.wait()


def pieces_of(start, end):
    found = []
    for part in range(DP):
        low, high = max(start, EMIT_START[part]), min(end, EMIT_END[part])
        if low < high:
            found.append((part, low - EMIT_START[part], low - start, high - low))
    return found


def lay_out_kernel(ag, w_in, m_in, v_in, norm, q_out, o_out, u_out, d_out, n_out, w_out, m_out, v_out, norm_out,
                   q_stage, out_sem, q_sem, flat_sem):
    def ranges(dst, start, end, base):
        return [pltpu.make_async_copy(ag.at[pl.ds(part * EMIT + low, count)], dst.at[pl.ds(offset, count)], out_sem.at[base + index])
                for index, (part, low, offset, count) in enumerate(pieces_of(start, end))]

    outs = []
    for dst, start, end in ((o_out, O_START, U_START), (u_out, U_START, D_START), (d_out, D_START, N_START)):
        outs += ranges(dst, start, end, len(outs))
    for index, (src, dst) in enumerate(((w_in, w_out), (m_in, m_out), (v_in, v_out))):
        outs.append(pltpu.make_async_copy(src, dst, flat_sem.at[index]))

    def q_store(block):
        return pltpu.make_async_copy(q_stage.at[:, lanes(block)], q_out.at[:, lanes(block)], q_sem.at[block])

    def row_start(row):
        start = row * Q_COLS
        for part in range(1, 4):
            gap = EMIT - (EMIT_END[part - 1] - EMIT_START[part - 1])
            start = start + jnp.where(row * Q_COLS >= EMIT_START[part], gap, 0)
        return start

    def turn(block):
        starts = [row_start(block * 16 + index) for index in range(16)]

        def body(group):
            for index in range(TURN_UNROLL):
                col = group * TURN_UNROLL + index
                part = jnp.concatenate([ag[start + col].astype(F32) for start in starts], axis=0)
                q_stage[lanes(col), lanes(block)] = part.T.astype(BF16)

        fori(Q_COLS // TURN_UNROLL, body)
        q_store(block).start()

    for copy in outs:
        copy.start()
    norm_out[0, 0] = jnp.max(norm[...])
    fori(8, turn)
    for col in range(M_COLS):
        n_out[:, col * 128:(col + 1) * 128] = ag[(DP - 1) * EMIT + N_START - EMIT_START[-1] + col].astype(F32)[:6].astype(BF16)
    for copy in outs:
        copy.wait()
    fori(8, lambda block: q_store(block).wait())


def to_tiles(matrix):
    rows, cols = matrix.shape
    return matrix.reshape(rows // 8, 8, cols // 128, 128).transpose(0, 2, 1, 3).reshape(rows * cols // 1024, 8, 128)


def from_tiles(tiles, rows, cols):
    return tiles.reshape(rows // 8, cols // 128, 8, 128).transpose(0, 2, 1, 3).reshape(rows, cols)


on_chip = pltpu.with_memory_space_constraint


def in_hbm(*arrays):
    return [on_chip(array, pltpu.HBM) for array in arrays]


def any_spec(count):
    return [pl.BlockSpec(memory_space=pltpu.HBM)] * count


def solution(mesh):
    dma = pltpu.SemaphoreType.DMA

    q_shape = (1920, 1024)
    params = functools.partial(pltpu.CompilerParams, vmem_limit_bytes=VMEM_LIMIT)

    def local_step(g_qkv, g_out, g_up, g_down, g_norms, master, mom_one, mom_two):
        gq = g_qkv[0].transpose(1, 2, 3, 0).reshape(q_shape)
        go, gu, gd = to_tiles(g_out[0]), to_tiles(g_up[0]), to_tiles(g_down[0])
        gn = g_norms[0]
        part = jax.ShapeDtypeStruct(master.shape, F32)
        flat = pltpu.VMEM((1, FLAT), F32)
        tile_count = (U_START - O_START, D_START - U_START, N_START - D_START)
        win_f32, half_f32 = pltpu.VMEM((WIN, *TILE), F32), pltpu.VMEM((HALF, *TILE), F32)
        half_bf16 = pltpu.VMEM((HALF, *TILE), BF16)
        scratch = [
            pltpu.VMEM((TILES, *TILE), BF16),
            pltpu.VMEM(q_shape, BF16),
            *[pltpu.VMEM((2, HALF, *TILE), BF16)] * 4,
            pltpu.VMEM((WIN, *TILE), BF16),
            half_bf16, half_bf16, half_f32, half_f32, half_f32, half_f32, win_f32, win_f32,
            pltpu.VMEM((3, STATE_ROWS, 128), F32),
            flat,
            *[pltpu.VMEM((1, HALO * 128), F32)] * 3,
            pltpu.VMEM(g_norms.shape[1:], BF16),
            pltpu.VMEM((WIN + 16, *TILE), BF16),
            pltpu.VMEM((DP, *TILE), F32),
            pltpu.VMEM((TP, *TILE), F32),
            dma((8,)), dma((3,)), dma(()), dma((SENDS,)),
            dma((4, K_RS)), dma((2 * K_RS,)), dma((2, K_RS)), dma((2, K_RS)), dma((3,)), dma(()), dma(()),
            dma((2, K_AG)), dma((K_AG,)), dma(()), dma((3,)),
        ]
        ag, w_new, m_new, v_new, norm = pl.pallas_call(
            step_kernel,
            name="reduce_update_gather",
            out_shape=[pltpu.VMEM((DP, EMIT, *TILE), BF16), flat, flat, flat,
                       pltpu.VMEM(TILE, F32)],
            in_specs=any_spec(8),
            out_specs=[pl.BlockSpec(memory_space=pl.ANY)] * 4 + [pl.BlockSpec(memory_space=pltpu.VMEM)],
            scratch_shapes=scratch,
            compiler_params=params(collective_id=0, has_side_effects=True, vmem_limit_bytes=STEP_VMEM),
        )(*in_hbm(gq, go, gu, gd, gn, master, mom_one, mom_two))
        pq, po, pu, pd, pn, w_new, m_new, v_new, norm = pl.pallas_call(
            lay_out_kernel,
            name="lay_out",
            out_shape=[jax.ShapeDtypeStruct(q_shape, BF16),
                       *[jax.ShapeDtypeStruct((count, *TILE), BF16) for count in tile_count],
                       jax.ShapeDtypeStruct(g_norms.shape[1:], BF16), part, part, part, jax.ShapeDtypeStruct((1, 1), F32)],
            in_specs=[pl.BlockSpec(memory_space=pltpu.VMEM)] * 5,
            out_specs=any_spec(4) + [pl.BlockSpec(memory_space=pltpu.VMEM)] + any_spec(3)
            + [pl.BlockSpec(memory_space=pltpu.SMEM)],
            scratch_shapes=[pltpu.VMEM(q_shape, BF16), dma((12,)), dma((8,)), dma((3,))],
            compiler_params=params(),
        )(*[on_chip(array, pltpu.VMEM) for array in (ag.reshape(DP * EMIT, *TILE), w_new, m_new, v_new, norm)])
        p_qkv = pq.reshape(8, 3, 80, 1024).transpose(3, 0, 1, 2)
        return (p_qkv, *[from_tiles(tiles, tiles.shape[0], 1024) for tiles in (po, pu, pd)],
                pn, w_new, m_new, v_new, norm[0, 0])

    return jax.shard_map(local_step, mesh=mesh, in_specs=ARG_SPECS, out_specs=OUT_SPECS, check_vma=False)
```

```python
import functools

import jax
import jax.numpy as jnp
from jax import lax
from jax.experimental import pallas as pl
from jax.experimental.pallas import tpu as pltpu
from jax.sharding import PartitionSpec as P

STEP = 20
BETA_ONE = 0.9
BETA_TWO = 0.95
ADAM_EPS = 1e-8
DECAY = 0.1
LEARN_RATE = 1e-4
MAX_NORM = 1.0
NORM_EPS = 1e-6
BIAS_ONE = 1.0 - BETA_ONE ** STEP
BIAS_TWO = 1.0 - BETA_TWO ** STEP
TP_COL = P(None, "tp")
ROW_DP = P("dp")
STATE = P("tp", "dp")
ARG_SPECS = (P("dp", None, "tp"), P("dp", "tp"), P("dp", None, "tp"), P("dp", "tp"), ROW_DP, STATE, STATE, STATE)
OUT_SPECS = (TP_COL, P("tp"), TP_COL, P("tp"), P(), STATE, STATE, STATE, P())

MESH = pl.DeviceIdType.MESH
F32 = jnp.float32
BF16 = jnp.bfloat16

Q_TILES = 1920
TILES = 4616
Q_COLS = 15
M_COLS = 8
PART_ROWS = 4614
MAT_ROWS = 36864
WIN = 600
HALF = WIN // 2
WIN_START = (0, 570, 1140, 1725, 2304, 2880, 3456, 4016)
EMIT_START = (0, 585, 1155, 1740, 2312, 2888, 3464, 4040)
EMIT_END = (585, 1155, 1740, 2312, 2888, 3464, 4040, 4616)
Q_BLOCKS = (40, 40, 40, 13, 0, 0, 0, 0)
M_BLOCKS = (0, 0, 0, 50, 75, 75, 75, 75)
EMIT = 588
STATE_BASE = 176
STATE_ROWS = 4984
HALO = 80

K_RS = 5
N_RS = HALF // K_RS
K_AG = 12
N_AG = EMIT // K_AG
STEP_TILES = 4
HALF_AG = K_AG // 2
FLAT = PART_ROWS * 128
CHUNK_ROWS = 64
CHUNK = CHUNK_ROWS * 128
CHUNKS = PART_ROWS // CHUNK_ROWS
TAIL = PART_ROWS - CHUNKS * CHUNK_ROWS
TILE = (8, 128)
TURN_UNROLL = 5
VMEM_LIMIT = 43 * 1024 * 1024
STEP_VMEM = 43 * 1024 * 1024
DP, TP = 8, 4
O_START, U_START, D_START, N_START = 1920, 2560, 3584, 4608
S_RAW, S_PF, S_PP, S_SUM, S_HALO, S_N1, S_N2, S_OWN, S_PAIR, S_PASS, SENDS = 0, 8, 9, 11, 13, 16, 17, 18, 21, 24, 25


def fori(count, step, start=0):
    def body(k, carry):
        step(k)
        return carry

    lax.fori_loop(start, count, body, 0)


def lanes(block):
    return pl.ds(pl.multiple_of(block * 128, 128), 128)


PIECE_ORDER = tuple(k // 2 + (K_AG // 2) * (k % 2) for k in range(K_AG))


def piece_blocks():
    table = []
    for k, piece in enumerate(PIECE_ORDER):
        rows = []
        for part in range(8):
            base = EMIT_START[part] - WIN_START[part]
            q_count, m_count = Q_BLOCKS[part], M_BLOCKS[part]

            def after(tile):
                q = min(q_count, max(0, -(-tile // Q_COLS)))
                m = min(m_count, max(0, -(-(tile - q_count * Q_COLS) // M_COLS)))
                return q, m

            def before(tile):
                q = min(q_count, max(0, tile // Q_COLS))
                m = min(m_count, max(0, (tile - q_count * Q_COLS) // M_COLS))
                return q, m

            middle = before(base + (K_AG // 2) * N_AG)
            low = (0, 0) if piece == 0 else middle if piece == K_AG // 2 else after(base + piece * N_AG)
            if piece == K_AG - 1:
                high = (q_count, m_count)
            elif piece == K_AG // 2 - 1:
                high = middle
            else:
                high = after(base + (piece + 1) * N_AG)
            rows.append((low[0], high[0], low[1], high[1]))
        table.append(tuple(zip(*rows)))
    return tuple(table)


PIECE_BLOCKS = piece_blocks()


def pick(values, y, x, c):
    total = 0
    for index, value in enumerate(values):
        if value:
            term = value
            for shift, bit in ((2, y), (1, x), (0, c)):
                term = term * (bit if (index >> shift) & 1 else 1 - bit)
            total = total + term
    return total


def step_kernel(gq, go, gu, gd, gn, w_in, m_in, v_in,
                ag, w_out, m_out, v_out, norm_out,
                grads, q_stage, r_ra, r_rb, r_da, r_db, r_pf, r_pa, r_pb,
                r_sa, r_sb, s_sa, s_sb, gsum, mask, state, flat_buf, halo_w, halo_m, halo_v,
                gn_stage, pbuf, nb1, nb2,
                load_sem, store_sem, own_sem, ss, rs_raw, rs_pf, rs_pp, rs_s, rs_h, rs_n1, rs_n2,
                rs_own, rs_pass, rs_own_pair, rs_pair):
    dp = lax.axis_index("dp")
    tp = lax.axis_index("tp")
    y = dp // 4
    x = dp // 2 % 2
    c = dp % 2

    def at(yy, xx, cc):
        return {"dp": yy * 4 + xx * 2 + cc}

    def win(yy, xx, cc):
        return pick(WIN_START, yy, xx, cc)

    ny, nx, nc = 1 - y, 1 - x, 1 - c

    def remote(src, dst, ssem, rsem, dev):
        return pltpu.make_async_remote_copy(
            src_ref=src, dst_ref=dst, send_sem=ssem, recv_sem=rsem, device_id=dev, device_id_type=MESH)

    halos = (halo_w, halo_m, halo_v)
    load_q = pltpu.make_async_copy(gq, q_stage, load_sem.at[0])
    loads = [pltpu.make_async_copy(gn, gn_stage, load_sem.at[1])]
    for index, (src, start, end) in enumerate(((go, O_START, U_START), (gu, U_START, D_START), (gd, D_START, N_START))):
        loads.append(pltpu.make_async_copy(src, grads.at[pl.ds(start, end - start)], load_sem.at[2 + index]))
    state_loads = [pltpu.make_async_copy(src, flat_buf, load_sem.at[5 + index])
                   for index, src in enumerate((w_in, m_in, v_in))]
    barrier = pltpu.get_barrier_semaphore()
    load_q.start()
    for copy in loads:
        copy.start()
    for offset in range(1, DP):
        pl.semaphore_signal(barrier, inc=1, device_id={"dp": (dp + offset) % DP}, device_id_type=MESH)
    for offset in range(1, TP):
        pl.semaphore_signal(barrier, inc=1, device_id={"tp": (tp + offset) % TP}, device_id_type=MESH)

    first = (4 - 4 * x) * y

    def turn(k):
        block = (k + first) % 8

        def body(col):
            turned = q_stage[lanes(col), lanes(block)].T
            for index in range(16):
                grads[block * 240 + index * Q_COLS + col] = turned[index * 8:(index + 1) * 8]

        fori(Q_COLS, body)

    load_q.wait()
    fori(2, turn)
    for copy in loads:
        copy.wait()
    for col in range(M_COLS):
        rows = gn_stage[:, col * 128:(col + 1) * 128].astype(F32)
        grads[N_START + col] = jnp.concatenate([rows, jnp.zeros((2, 128), F32)], axis=0).astype(BF16)
    pl.semaphore_wait(barrier, DP + TP - 2)

    def cut(start, k, n=N_RS):
        return pl.ds(start + k * n, n)

    raw_bufs = (r_ra, r_rb, r_da, r_db)

    def raw(stream, cc, k):
        to_y = stream in (0, 2)
        half = 0 if to_y else HALF
        if stream < 2:
            start = win(ny, nx, cc)
        elif to_y:
            start = win(ny, x, cc)
        else:
            start = win(y, nx, cc)
        dev = at(ny, x, cc) if to_y else at(y, nx, cc)
        return remote(grads.at[cut(start + half, k)], raw_bufs[stream].at[c, cut(0, k)],
                      ss.at[S_RAW + 2 * stream + cc], rs_raw.at[stream, k], dev)

    partner = at(y, x, nc)

    def partner_final(k):
        return remote(grads.at[cut(win(y, x, nc), k)], r_pf.at[cut(0, k)], ss.at[S_PF], rs_pf.at[k], partner)

    def partner_relay(which, k):
        if which == 0:
            start, dst = win(y, nx, nc), r_pa
        else:
            start, dst = win(ny, x, nc) + HALF, r_pb
        return remote(grads.at[cut(start, k)], dst.at[cut(0, k)], ss.at[S_PP + which], rs_pp.at[which, k], partner)

    def relayed(which, k):
        src, dst, dev = (s_sa, r_sa, at(y, nx, c)) if which == 0 else (s_sb, r_sb, at(ny, x, c))
        return remote(src.at[cut(0, k)], dst.at[cut(0, k)], ss.at[S_SUM + which], rs_s.at[which, k], dev)

    def halo_copy(index):
        src = (w_in, m_in, v_in)[index]
        return remote(src.at[:, pl.ds(0, HALO * 128)], halos[index],
                      ss.at[S_HALO + index], rs_h.at[index], {"dp": (dp + DP - 1) % DP})

    def arrived(buf, sem):
        pltpu.make_async_copy(buf, buf, sem).wait()

    def sent(buf, sem):
        pltpu.make_async_copy(buf, buf, sem).wait()

    def raw_arrived(stream, k):
        arrived(raw_bufs[stream].at[:, cut(0, k)], rs_raw.at[stream, k])

    def send_diag(*which):
        def step(k):
            for stream, cc in which:
                raw(stream, cc, k).start()
        fori(K_RS, step)

    def send_over_y(k):
        raw(2, 0, k).start()
        raw(2, 1, k).start()
        partner_relay(1, k).start()

    def send_over_x(k):
        raw(3, 0, k).start()
        raw(3, 1, k).start()
        partner_relay(0, k).start()
        partner_final(k).start()
        partner_final(k + K_RS).start()

    @pl.when(y == 0)
    def _():
        send_diag((0, 0), (1, 0), (0, 1), (1, 1))
        fori(K_RS, send_over_y)
        fori(8, turn, 2)
        fori(K_RS, send_over_x)

    @pl.when(y == 1)
    def _():
        send_diag((0, 0))
        fori(K_RS, send_over_x)
        fori(5, turn, 2)
        send_diag((0, 1), (1, 0), (1, 1))
        fori(8, turn, 5)
        fori(K_RS, send_over_y)

    for index in range(3):
        halo_copy(index).start()
    state_loads[0].start()

    off = PART_ROWS * dp - 8 * win(y, x, c)
    mat_end = MAT_ROWS - 8 * win(y, x, c)
    last = jnp.minimum(off + PART_ROWS, mat_end + jnp.where(tp == 0, 48, 0))
    q_blocks = pick(Q_BLOCKS, y, x, c)
    m_blocks = pick(M_BLOCKS, y, x, c)
    row = lax.broadcasted_iota(jnp.int32, TILE, 0)
    mask[pl.ds(WIN - 5, 5)] = jnp.zeros((5, *TILE), F32)

    def mask_blocks(columns, tile0):
        def body(block):
            for col in range(columns):
                tile = tile0 + block * columns + col
                lane_row = row * columns + (tile0 * 8 + block * columns * 8 + col)
                inside = jnp.logical_and(lane_row >= off, lane_row < last)
                mask[tile] = jnp.where(inside, 1.0, 0.0)
        return body

    fori(q_blocks, mask_blocks(Q_COLS, 0))
    fori(m_blocks, mask_blocks(M_COLS, q_blocks * Q_COLS))

    def flat_part(k):
        return pl.ds(pl.multiple_of(k * CHUNK, CHUNK), CHUNK)

    def row_part(k):
        return pl.ds(STATE_BASE + k * CHUNK_ROWS, CHUNK_ROWS)

    tail_flat = pl.ds(CHUNKS * CHUNK, TAIL * 128)
    tail_rows = pl.ds(STATE_BASE + CHUNKS * CHUNK_ROWS, TAIL)

    for index in range(3):
        def to_rows(k):
            state[index, row_part(k)] = flat_buf[:, flat_part(k)].reshape(CHUNK_ROWS, 128)

        state_loads[index].wait()
        fori(CHUNKS, to_rows)
        state[index, tail_rows] = flat_buf[:, tail_flat].reshape(TAIL, 128)
        if index < 2:
            state_loads[index + 1].start()

    def relay(which):
        own_start = win(y, nx, c) if which == 0 else win(ny, x, c) + HALF
        raw_buf, pair_buf, out_buf = (r_ra, r_pa, s_sa) if which == 0 else (r_rb, r_pb, s_sb)

        def body(k):
            raw_arrived(which, k)
            arrived(pair_buf.at[cut(0, k)], rs_pp.at[which, k])

            def tiles(index):
                here = pl.ds(k * N_RS + index * STEP_TILES, STEP_TILES)
                total = grads[pl.ds(own_start + k * N_RS + index * STEP_TILES, STEP_TILES)].astype(F32)
                total = total + pair_buf[here].astype(F32)
                total = total + raw_buf[0, here].astype(F32)
                total = total + raw_buf[1, here].astype(F32)
                out_buf[here] = total

            fori(N_RS // STEP_TILES, tiles)
            relayed(which, k).start()
        return body

    relay_a, relay_b = relay(0), relay(1)

    def relay_step(k):
        relay_a(k)
        relay_b(k)

    fori(K_RS, relay_step)

    for index in range(3):
        arrived(halos[index], rs_h.at[index])
        state[index, pl.ds(STATE_BASE + PART_ROWS, HALO)] = halos[index][...].reshape(HALO, 128)

    def finish(which):
        half = 0 if which == 0 else HALF
        raw_buf, sum_buf = (r_da, r_sa) if which == 0 else (r_db, r_sb)

        def body(k, acc):
            raw_arrived(2 + which, k)
            arrived(r_pf.at[cut(half, k)], rs_pf.at[k + which * K_RS])
            arrived(sum_buf.at[cut(0, k)], rs_s.at[which, k])

            def tiles(index, acc):
                here = pl.ds(k * N_RS + index * STEP_TILES, STEP_TILES)
                part = pl.ds(half + k * N_RS + index * STEP_TILES, STEP_TILES)
                total = grads[pl.ds(win(y, x, c) + half + k * N_RS + index * STEP_TILES, STEP_TILES)].astype(F32)
                total = total + r_pf[part].astype(F32)
                total = total + raw_buf[0, here].astype(F32)
                total = total + raw_buf[1, here].astype(F32)
                total = (total + sum_buf[here]) * 0.125
                gsum[part] = total
                square = jnp.where(mask[part] > 0.5, total * total, 0.0)
                return acc + jnp.sum(square, axis=0)

            return lax.fori_loop(0, N_RS // STEP_TILES, tiles, acc)
        return body

    finish_a, finish_b = finish(0), finish(1)
    acc = lax.fori_loop(0, K_RS, lambda k, acc: finish_b(k, finish_a(k, acc)), jnp.zeros(TILE, F32))

    nb1[dp] = acc

    for offset in range(1, DP):
        remote(nb1.at[dp], nb1.at[dp], ss.at[S_N1], rs_n1, {"dp": (dp + offset) % DP}).start()
    arrived(nb1.at[pl.ds(0, DP - 1)], rs_n1)
    plane = nb1[0]
    for index in range(1, DP):
        plane = plane + nb1[index]
    nb2[tp] = plane
    for offset in range(1, TP):
        remote(nb2.at[tp], nb2.at[tp], ss.at[S_N2], rs_n2, {"tp": (tp + offset) % TP}).start()
    arrived(nb2.at[pl.ds(0, TP - 1)], rs_n2)
    total = nb2[0] + nb2[1] + nb2[2] + nb2[3]
    total = jnp.sum(jnp.sum(total, axis=0, keepdims=True), axis=1, keepdims=True)
    norm = jnp.sqrt(jnp.broadcast_to(total, TILE))
    norm_out[...] = norm
    clip = jnp.minimum(1.0, MAX_NORM / (norm + NORM_EPS))

    def update_blocks(columns, tile0):
        def body(block):
            row0 = tile0 * 8 + block * columns * 8
            decay = jnp.where(row0 < mat_end, DECAY, 0.0)
            for col in range(columns):
                tile = tile0 + block * columns + col
                here = pl.ds(STATE_BASE - off + row0 + col, 8, stride=columns)
                grad = gsum[tile] * clip
                w_old = state[0, here]
                m_new = BETA_ONE * state[1, here] + (1.0 - BETA_ONE) * grad
                v_new = BETA_TWO * state[2, here] + (1.0 - BETA_TWO) * grad * grad
                step_dir = (m_new * (1.0 / BIAS_ONE)) / (jnp.sqrt(v_new * (1.0 / BIAS_TWO)) + ADAM_EPS)
                w_new = w_old - LEARN_RATE * (step_dir + decay * w_old)
                state[0, here] = w_new
                state[1, here] = m_new
                state[2, here] = v_new
                pbuf[tile] = w_new.astype(BF16)
        return body

    update_q = update_blocks(Q_COLS, 0)
    update_m = update_blocks(M_COLS, q_blocks * Q_COLS)

    emit0 = pick([e - s for e, s in zip(EMIT_START, WIN_START)], y, x, c)

    def piece(k):
        return pl.ds(k * N_AG, N_AG)

    part_x, part_y, part_d = y * 4 + nx * 2 + c, ny * 4 + x * 2 + c, ny * 4 + nx * 2 + c
    dev_x, dev_y = at(y, nx, c), at(ny, x, c)

    def own_out(which, k):
        dev = (dev_x, dev_y, partner)[which]
        rsem = rs_own_pair if which == 2 else rs_own.at[which, k]
        return remote(pbuf.at[pl.ds(emit0 + k * N_AG, N_AG)], ag.at[dp, piece(k)], ss.at[S_OWN + which], rsem, dev)

    def pass_out(which, k):
        part, dev = ((part_x, dev_y), (part_y, dev_x))[which]
        return remote(ag.at[part, piece(k)], ag.at[part, piece(k)], ss.at[S_PASS], rs_pass.at[k], dev)

    def pair_out(which, k):
        part = (part_x, part_y, part_d)[which]
        return remote(ag.at[part, piece(k)], ag.at[part, piece(k)], ss.at[S_PAIR + which], rs_pair.at[which], partner)

    own_copy = pltpu.make_async_copy(pbuf.at[pl.ds(emit0, EMIT)], ag.at[dp], own_sem)

    for k, bounds in enumerate(PIECE_BLOCKS):
        q_from, q_to, m_from, m_to = (pick(bound, y, x, c) for bound in bounds)
        fori(q_to, update_q, q_from)
        fori(m_to, update_m, m_from)
        own_out(k % 2, PIECE_ORDER[k]).start()
        own_out(2, PIECE_ORDER[k]).start()

    def send_rest(k):
        own_out(0, HALF_AG + k).start()
        own_out(1, k).start()

    fori(HALF_AG, send_rest)
    own_copy.start()

    def store_state(index):
        def to_flat(k):
            flat_buf[:, flat_part(k)] = state[index, row_part(k)].reshape(1, CHUNK)

        fori(CHUNKS, to_flat)
        flat_buf[:, tail_flat] = state[index, tail_rows].reshape(1, TAIL * 128)
        copy = pltpu.make_async_copy(flat_buf, (w_out, m_out, v_out)[index], store_sem.at[index])
        copy.start()
        return copy

    def first_half(k):
        arrived(ag.at[part_x, piece(k)], rs_own.at[0, k])
        pass_out(0, k).start()
        pair_out(0, k).start()
        later = k + HALF_AG
        arrived(ag.at[part_y, piece(later)], rs_own.at[1, later])
        pass_out(1, later).start()
        pair_out(1, later).start()

    def second_half(k):
        later = k + HALF_AG
        arrived(ag.at[part_x, piece(later)], rs_own.at[0, later])
        pair_out(0, later).start()
        arrived(ag.at[part_y, piece(k)], rs_own.at[1, k])
        pair_out(1, k).start()

    def diagonal(k):
        for index in (k, k + HALF_AG):
            arrived(ag.at[part_d, piece(index)], rs_pass.at[index])
            pair_out(2, index).start()

    for index, step in enumerate((first_half, second_half, diagonal)):
        store = store_state(index)
        fori(HALF_AG, step)
        store.wait()

    for stream in range(4):
        for cc in range(2):
            sent(raw_bufs[stream].at[0], ss.at[S_RAW + 2 * stream + cc])
    sent(r_pf, ss.at[S_PF])
    for which in range(2):
        sent(r_pa, ss.at[S_PP + which])
        sent(s_sa, ss.at[S_SUM + which])
    for which in range(3):
        sent(halos[which], ss.at[S_HALO + which])
        sent(ag.at[0], ss.at[S_OWN + which])
        sent(ag.at[0], ss.at[S_PAIR + which])
    sent(nb1.at[pl.ds(0, DP - 1)], ss.at[S_N1])
    sent(nb2.at[pl.ds(0, TP - 1)], ss.at[S_N2])
    sent(ag.at[0], ss.at[S_PASS])
    arrived(ag.at[y * 4 + x * 2 + nc], rs_own_pair)
    for which, part in enumerate((y * 4 + nx * 2 + nc, ny * 4 + x * 2 + nc, ny * 4 + nx * 2 + nc)):
        arrived(ag.at[part], rs_pair.at[which])
    own_copy.wait()


def pieces_of(start, end):
    found = []
    for part in range(DP):
        low, high = max(start, EMIT_START[part]), min(end, EMIT_END[part])
        if low < high:
            found.append((part, low - EMIT_START[part], low - start, high - low))
    return found


def lay_out_kernel(ag, w_in, m_in, v_in, norm, q_out, o_out, u_out, d_out, n_out, w_out, m_out, v_out, norm_out,
                   q_stage, out_sem, q_sem, flat_sem):
    def ranges(dst, start, end, base):
        return [pltpu.make_async_copy(ag.at[pl.ds(part * EMIT + low, count)], dst.at[pl.ds(offset, count)], out_sem.at[base + index])
                for index, (part, low, offset, count) in enumerate(pieces_of(start, end))]

    outs = []
    for dst, start, end in ((o_out, O_START, U_START), (u_out, U_START, D_START), (d_out, D_START, N_START)):
        outs += ranges(dst, start, end, len(outs))
    for index, (src, dst) in enumerate(((w_in, w_out), (m_in, m_out), (v_in, v_out))):
        outs.append(pltpu.make_async_copy(src, dst, flat_sem.at[index]))

    def q_store(block):
        return pltpu.make_async_copy(q_stage.at[:, lanes(block)], q_out.at[:, lanes(block)], q_sem.at[block])

    def row_start(row):
        start = row * Q_COLS
        for part in range(1, 4):
            gap = EMIT - (EMIT_END[part - 1] - EMIT_START[part - 1])
            start = start + jnp.where(row * Q_COLS >= EMIT_START[part], gap, 0)
        return start

    def turn(block):
        starts = [row_start(block * 16 + index) for index in range(16)]

        def body(group):
            for index in range(TURN_UNROLL):
                col = group * TURN_UNROLL + index
                part = jnp.concatenate([ag[start + col].astype(F32) for start in starts], axis=0)
                q_stage[lanes(col), lanes(block)] = part.T.astype(BF16)

        fori(Q_COLS // TURN_UNROLL, body)
        q_store(block).start()

    for copy in outs:
        copy.start()
    norm_out[0, 0] = jnp.max(norm[...])
    fori(8, turn)
    for col in range(M_COLS):
        n_out[:, col * 128:(col + 1) * 128] = ag[(DP - 1) * EMIT + N_START - EMIT_START[-1] + col].astype(F32)[:6].astype(BF16)
    for copy in outs:
        copy.wait()
    fori(8, lambda block: q_store(block).wait())


def to_tiles(matrix):
    rows, cols = matrix.shape
    return matrix.reshape(rows // 8, 8, cols // 128, 128).transpose(0, 2, 1, 3).reshape(rows * cols // 1024, 8, 128)


def from_tiles(tiles, rows, cols):
    return tiles.reshape(rows // 8, cols // 128, 8, 128).transpose(0, 2, 1, 3).reshape(rows, cols)


on_chip = pltpu.with_memory_space_constraint


def in_hbm(*arrays):
    return [on_chip(array, pltpu.HBM) for array in arrays]


def any_spec(count):
    return [pl.BlockSpec(memory_space=pltpu.HBM)] * count


def solution(mesh):
    dma = pltpu.SemaphoreType.DMA

    q_shape = (1920, 1024)
    params = functools.partial(pltpu.CompilerParams, vmem_limit_bytes=VMEM_LIMIT)

    def local_step(g_qkv, g_out, g_up, g_down, g_norms, master, mom_one, mom_two):
        gq = g_qkv[0].transpose(1, 2, 3, 0).reshape(q_shape)
        go, gu, gd = to_tiles(g_out[0]), to_tiles(g_up[0]), to_tiles(g_down[0])
        gn = g_norms[0]
        part = jax.ShapeDtypeStruct(master.shape, F32)
        flat = pltpu.VMEM((1, FLAT), F32)
        tile_count = (U_START - O_START, D_START - U_START, N_START - D_START)
        win_f32, half_f32 = pltpu.VMEM((WIN, *TILE), F32), pltpu.VMEM((HALF, *TILE), F32)
        half_bf16 = pltpu.VMEM((HALF, *TILE), BF16)
        scratch = [
            pltpu.VMEM((TILES, *TILE), BF16),
            pltpu.VMEM(q_shape, BF16),
            *[pltpu.VMEM((2, HALF, *TILE), BF16)] * 4,
            pltpu.VMEM((WIN, *TILE), BF16),
            half_bf16, half_bf16, half_f32, half_f32, half_f32, half_f32, win_f32, win_f32,
            pltpu.VMEM((3, STATE_ROWS, 128), F32),
            flat,
            *[pltpu.VMEM((1, HALO * 128), F32)] * 3,
            pltpu.VMEM(g_norms.shape[1:], BF16),
            pltpu.VMEM((WIN + 16, *TILE), BF16),
            pltpu.VMEM((DP, *TILE), F32),
            pltpu.VMEM((TP, *TILE), F32),
            dma((8,)), dma((3,)), dma(()), dma((SENDS,)),
            dma((4, K_RS)), dma((2 * K_RS,)), dma((2, K_RS)), dma((2, K_RS)), dma((3,)), dma(()), dma(()),
            dma((2, K_AG)), dma((K_AG,)), dma(()), dma((3,)),
        ]
        ag, w_new, m_new, v_new, norm = pl.pallas_call(
            step_kernel,
            name="reduce_update_gather",
            out_shape=[pltpu.VMEM((DP, EMIT, *TILE), BF16), flat, flat, flat,
                       pltpu.VMEM(TILE, F32)],
            in_specs=any_spec(8),
            out_specs=[pl.BlockSpec(memory_space=pl.ANY)] * 4 + [pl.BlockSpec(memory_space=pltpu.VMEM)],
            scratch_shapes=scratch,
            compiler_params=params(collective_id=0, has_side_effects=True, vmem_limit_bytes=STEP_VMEM),
        )(*in_hbm(gq, go, gu, gd, gn, master, mom_one, mom_two))
        pq, po, pu, pd, pn, w_new, m_new, v_new, norm = pl.pallas_call(
            lay_out_kernel,
            name="lay_out",
            out_shape=[jax.ShapeDtypeStruct(q_shape, BF16),
                       *[jax.ShapeDtypeStruct((count, *TILE), BF16) for count in tile_count],
                       jax.ShapeDtypeStruct(g_norms.shape[1:], BF16), part, part, part, jax.ShapeDtypeStruct((1, 1), F32)],
            in_specs=[pl.BlockSpec(memory_space=pltpu.VMEM)] * 5,
            out_specs=any_spec(4) + [pl.BlockSpec(memory_space=pltpu.VMEM)] + any_spec(3)
            + [pl.BlockSpec(memory_space=pltpu.SMEM)],
            scratch_shapes=[pltpu.VMEM(q_shape, BF16), dma((12,)), dma((8,)), dma((3,))],
            compiler_params=params(),
        )(*[on_chip(array, pltpu.VMEM) for array in (ag.reshape(DP * EMIT, *TILE), w_new, m_new, v_new, norm)])
        p_qkv = pq.reshape(8, 3, 80, 1024).transpose(3, 0, 1, 2)
        return (p_qkv, *[from_tiles(tiles, tiles.shape[0], 1024) for tiles in (po, pu, pd)],
                pn, w_new, m_new, v_new, norm[0, 0])

    return jax.shard_map(local_step, mesh=mesh, in_specs=ARG_SPECS, out_specs=OUT_SPECS, check_vma=False)
```
